32 devices in a mesh: gx: 2 (over y), gy: 4 (over z), gz: 4 (over x, core).
Axes of the slice: x: 2, y: 2, z: 4, core: 2. Of those that a mesh axis runs over, the one named last changes fastest.
Arguments:
- fields: bfloat16 [384, 4, 16, 512], P(None, 'gx', 'gy', 'gz'), may hold values from -6 to 6
- trace_old: float32 [3, 32, 4, 16, 512], P(None, None, 'gx', 'gy', 'gz'), may hold values from -4 to 4
- face_load: float32 [3, 32, 4, 16, 512], P(None, None, 'gx', 'gy', 'gz'), may hold values from -6 to 6
- face_diag: float32 [3, 4, 16, 512], P(None, 'gx', 'gy', 'gz'), may hold values from 0.5 to 4
- fine_flag: int32 [4, 16, 512], P('gx', 'gy', 'gz'), may hold values from 0 to 1
- coeff: float32 [4, 16, 512], P('gx', 'gy', 'gz'), may hold values from 0.5 to 8
- volume_op: bfloat16 [384, 384], replicated, may hold values from -0.3125 to 0.3125
- lift_op: bfloat16 [384, 192], replicated, may hold values from -0.4375 to 0.4375
- schur_op: float32 [192, 192], replicated, may hold values from -8 to 8.5, as said below
Outputs:
- fields_new: bfloat16 [384, 4, 16, 512], P(None, 'gx', 'gy', 'gz')
- trace_new: float32 [3, 32, 4, 16, 512], P(None, None, 'gx', 'gy', 'gz')
The draws below stay inside these ranges and needn't reach their ends.
Inputs may be any that keep to these rules, and one draw needn't show every extreme that they name: schur_op is symmetric and positive definite.
All inputs are finite; a program needn't handle non-finite values.
Results may differ from the reference program's by a relative error of at most 0.0013.
Values sent between devices are 32-bit elements; how exact they have to be, the bound alone decides.
No kernel may reach another device: no remote copies, remote signals or barrier semaphores. Data moves between devices by JAX's collectives and lax.ppermute only.
A program may use at most 64 MiB of HBM per device.

```python
import math
import jax
import jax.numpy as jnp
from jax import lax

EX = 2
EY = 4
EZ = 128
ELEMDOF = 384
FACEDOF = 32
ITERS = 2
SCHUR = 192
NX = 4
NY = 16
NZ = 512


def draw_fine_flag(key, part):
    level_key, roll_key = jax.random.split(jax.random.fold_in(key, 17))
    levels = jax.random.randint(level_key, (NX // EX, NY // EY, NZ // EZ), 1, 10)
    spread = jnp.repeat(jnp.repeat(jnp.repeat(levels, EX, 0), EY, 1), EZ, 2)
    dice_rolls = jax.random.randint(roll_key, (NX, NY, NZ), 0, 10)
    return (dice_rolls < spread).astype(jnp.int32)


def draw_schur_op(key, part):
    base_key = jax.random.fold_in(key, 29)
    factor = jnp.clip(jax.random.normal(base_key, (SCHUR, SCHUR), jnp.float32), -4.0, 4.0)
    factor = factor / jnp.sqrt(jnp.float32(SCHUR))
    product = jnp.dot(factor, factor.T, precision=lax.Precision.HIGHEST)
    product = 0.5 * (product + product.T)
    return 0.5 * product + 0.5 * jnp.eye(SCHUR, dtype=jnp.float32)


def block_levels(stream_key, shape, shards, least, top_value):
    def one(axis_at, parts):
        draws = jax.random.uniform(jax.random.fold_in(jax.random.fold_in(stream_key, 6), axis_at), (parts,), jnp.float32, least / len(shards), top_value / len(shards))
        return jnp.repeat(jnp.exp(draws), shape[axis_at] // parts).reshape((-1,) + (1,) * (len(shape) - axis_at - 1))

    loudness = one(*shards[0])
    for cut in shards[1:]:
        loudness = loudness * one(*cut)
    return loudness


def bell_draw(stream_key, extent, deviation, limit, cuts=(), held_as=jnp.bfloat16):
    drawn = deviation * jax.random.normal(stream_key, extent, jnp.float32)
    if cuts:
        drawn = drawn * block_levels(stream_key, extent, cuts, -0.22, 0.18)
    return jnp.clip(drawn, -limit, limit).astype(held_as)


def setup_inputs(seed: int = 0) -> dict:
    arg_keys = jax.random.split(jax.random.key(seed), 10)
    return {
        "fields": bell_draw(arg_keys[0], (ELEMDOF, NX, NY, NZ), 1.0, 6.0, ((1, 2), (2, 4), (3, 4))),
        "trace_old": bell_draw(arg_keys[1], (3, FACEDOF, NX, NY, NZ), 0.5, 4.0, ((2, 2), (3, 4), (4, 4)), jnp.float32),
        "face_load": bell_draw(arg_keys[2], (3, FACEDOF, NX, NY, NZ), 1.0, 6.0, ((2, 2), (3, 4), (4, 4)), jnp.float32),
        "face_diag": jnp.clip(jnp.exp(math.log(4.0) - 2.0794415 * jax.random.uniform(arg_keys[3], (3, NX, NY, NZ), jnp.float32) ** block_levels(arg_keys[3], (3, NX, NY, NZ), ((1, 2), (2, 4), (3, 4)), -0.2, 0.2)), 0.5, 4.0),
        "fine_flag": draw_fine_flag(jax.random.fold_in(arg_keys[9], 71), 0),
        "coeff": jnp.clip(jnp.exp(math.log(8.0) - 2.7725887 * jax.random.uniform(arg_keys[5], (NX, NY, NZ), jnp.float32) ** block_levels(arg_keys[5], (NX, NY, NZ), ((0, 2), (1, 4), (2, 4)), -0.2, 0.2)), 0.5, 8.0),
        "volume_op": bell_draw(arg_keys[6], (ELEMDOF, ELEMDOF), ELEMDOF ** -0.5, 0.3125),
        "lift_op": bell_draw(arg_keys[7], (ELEMDOF, SCHUR), SCHUR ** -0.5, 0.4375),
        "schur_op": draw_schur_op(jax.random.fold_in(arg_keys[9], 71), 0),
    }


time_step = 0.25
highest = lax.Precision.HIGHEST


def pad_upper(traces):
    return jnp.pad(traces, ((0, 0), (0, 0), (0, 1), (0, 1), (0, 1)))


def element_faces(padded, position):
    current = lax.dynamic_index_in_dim(padded, position, 2, keepdims=False)
    following = lax.dynamic_index_in_dim(padded, position + 1, 2, keepdims=False)
    pieces = [current[0, :, :NY, :NZ], following[0, :, :NY, :NZ],
              current[1, :, :NY, :NZ], current[1, :, 1:, :NZ],
              current[2, :, :NY, :NZ], current[2, :, :NY, 1:]]
    return jnp.concatenate(pieces, 0).reshape(SCHUR, NY * NZ)


def operate(traces, weight, face_diag, schur_op):
    padded = pad_upper(traces)

    def one_slab(position):
        face_values = element_faces(padded, position)
        applied = jnp.dot(schur_op, face_values, precision=highest, preferred_element_type=jnp.float32)
        element_weight = lax.dynamic_index_in_dim(weight, position, 0, keepdims=False).reshape(1, NY * NZ)
        return (applied * element_weight).reshape(6, FACEDOF, NY, NZ)

    images = lax.map(one_slab, jnp.arange(NX).astype(jnp.int32))
    along_x = images[:, 0] + jnp.concatenate([jnp.zeros_like(images[:1, 1]), images[:-1, 1]], 0)
    along_y = images[:, 2] + jnp.pad(images[:, 3], ((0, 0), (0, 0), (1, 0), (0, 0)))[:, :, :NY]
    along_z = images[:, 4] + jnp.pad(images[:, 5], ((0, 0), (0, 0), (0, 0), (1, 0)))[:, :, :, :NZ]
    coupled = jnp.stack([along_x, along_y, along_z], 0).transpose(0, 2, 1, 3, 4)
    return face_diag[:, None] * traces + coupled


def reference(fields, trace_old, face_load, face_diag, fine_flag, coeff, volume_op, lift_op, schur_op):
    fine_mask = fine_flag.astype(jnp.float32)
    weight = fine_mask * coeff
    solution = trace_old
    residual = face_load - operate(trace_old, weight, face_diag, schur_op)
    direction = residual
    norm_now = jnp.sum(residual * residual)
    for iteration in range(ITERS):
        applied = operate(direction, weight, face_diag, schur_op)
        step_length = norm_now / jnp.sum(direction * applied)
        solution = solution + step_length * direction
        if iteration + 1 < ITERS:
            residual = residual - step_length * applied
            norm_next = jnp.sum(residual * residual)
            direction = residual + (norm_next / norm_now) * direction
            norm_now = norm_next
    old_padded = pad_upper(trace_old)
    new_padded = pad_upper(solution)

    def update(position):
        nodal = lax.dynamic_index_in_dim(fields, position, 1, keepdims=False).reshape(ELEMDOF, NY * NZ)
        fine_row = lax.dynamic_index_in_dim(fine_mask, position, 0, keepdims=False).reshape(1, NY * NZ)
        traced = fine_row * element_faces(new_padded, position) + (1.0 - fine_row) * element_faces(old_padded, position)
        volume = jnp.dot(volume_op, nodal, preferred_element_type=jnp.float32)
        lifted = jnp.dot(lift_op, traced.astype(jnp.bfloat16), preferred_element_type=jnp.float32)
        result = nodal.astype(jnp.float32) + time_step * ((1.0 - fine_row) * volume + lifted)
        return result.astype(jnp.bfloat16).reshape(ELEMDOF, NY, NZ)

    updated = lax.map(update, jnp.arange(NX).astype(jnp.int32))
    return updated.transpose(1, 0, 2, 3), solution
```

```python
import functools

import jax
import jax.numpy as jnp
from jax import lax
from jax.experimental import pallas as pl
from jax.experimental.pallas import tpu as pltpu
from jax.sharding import PartitionSpec as P

AXES = ("gx", "gy", "gz")
TIME_STEP = 0.25
SHIFT_LIMIT = 1e4
VMEM_GRANT = 12 * 1024 * 1024
f32, bf16 = jnp.float32, jnp.bfloat16


def pairs(axis, odd):
    size = lax.axis_size(axis)
    route = []
    for i in range(odd, size - 1, 2):
        route += [(i, i + 1), (i + 1, i)]
    return route


def exchange(sends):
    got = []
    for axis, per_axis in zip(AXES, sends):
        got.append([lax.ppermute(v, axis, pairs(axis, odd)) if pairs(axis, odd) else None for odd, v in enumerate(per_axis)])
    return got


def counts():
    return [sum(bool(pairs(axis, odd)) for odd in (0, 1)) for axis in AXES]


def lane_iota(shape):
    return lax.broadcasted_iota(jnp.int32, shape, len(shape) - 1)


def moved(value, source, target):
    width = value.shape[-1]
    shift = (target - source) % width
    return pltpu.roll(value, shift, value.ndim - 1) if shift else value


def place():
    index = [lax.axis_index(a) for a in AXES]
    parity = [lax.rem(i, 2) for i in index]
    below_top = [(i < lax.axis_size(a) - 1).astype(f32) for i, a in zip(index, AXES)]
    return parity, below_top


def split(value):
    high = value.astype(bf16)
    return high, (value - high.astype(f32)).astype(bf16)


class Geometry:
    def __init__(self, F, EX, EY, EZ):
        self.F, self.EX, self.EY, self.EZ = F, EX, EY, EZ
        self.M = EX * EY


def gather_and_apply(geo, own, halo, schur, ghi, glo):
    F, EX, EY, EZ, M = geo.F, geo.EX, geo.EY, geo.EZ, geo.M
    hx, hy, hz = halo
    lanes = lane_iota((F, EZ))
    for m in range(M):
        i, j = divmod(m, EY)
        z_own = own(2, m)
        z_up = jnp.where(lanes == EZ - 1, moved(hz, m, EZ - 1), moved(z_own, 1, 0))
        blocks = [
            own(0, m), own(0, m + EY) if i + 1 < EX else hx(j),
            own(1, m), own(1, m + 1) if j + 1 < EY else hy(i),
            z_own, z_up,
        ]
        for s, block in enumerate(blocks):
            high, low = split(block)
            ghi[s * F:(s + 1) * F, m * EZ:(m + 1) * EZ] = high
            glo[s * F:(s + 1) * F, m * EZ:(m + 1) * EZ] = low
    n = 6 * F
    both = jnp.dot(schur[...], ghi[...], preferred_element_type=f32)
    return both[:n] + (both[n:] + jnp.dot(schur[:n], glo[...], preferred_element_type=f32))


def spread(geo, y, weight, own_term, sign, out, sends, parity):
    F, EX, EY, EZ, M = geo.F, geo.EX, geo.EY, geo.EZ, geo.M
    lanes = lane_iota((F, EZ))
    wrow = [weight[m:m + 1] * sign for m in range(M)]

    def block(s, m):
        return y[s * F:(s + 1) * F, m * EZ:(m + 1) * EZ] * wrow[m]

    low = {}
    bottom_z = jnp.zeros((F, EZ), f32)
    top_z = jnp.zeros((F, EZ), f32)
    for m in range(M):
        i, j = divmod(m, EY)
        vx = own_term(0, m) + block(0, m)
        if i > 0:
            vx = vx + block(1, m - EY)
        else:
            low[0, j] = vx
        out[0, m] = vx
        vy = own_term(1, m) + block(2, m)
        if j > 0:
            vy = vy + block(3, m - 1)
        else:
            low[1, i] = vy
        out[1, m] = vy
        up = block(5, m)
        vz = own_term(2, m) + block(4, m) + jnp.where(lanes == 0, 0.0, moved(up, 0, 1))
        out[2, m] = vz
        bottom_z = jnp.where(lanes == m, moved(vz, 0, m), bottom_z)
        top_z = jnp.where(lanes == m, moved(up, EZ - 1, m), top_z)
    high_x = [block(1, (EX - 1) * EY + j) for j in range(EY)]
    high_y = [block(3, i * EY + EY - 1) for i in range(EX)]
    for odd, ref in enumerate(sends[0]):
        for j in range(EY):
            ref[j] = jnp.where(parity[0] == odd, high_x[j], low[0, j])
    for odd, ref in enumerate(sends[1]):
        for i in range(EX):
            ref[i] = jnp.where(parity[1] == odd, high_y[i], low[1, i])
    for odd, ref in enumerate(sends[2]):
        ref[...] = jnp.where(parity[2] == odd, top_z, bottom_z)


def chosen(refs, parity, read, flip=False):
    values = [read(r) for r in refs]
    if not values:
        return None
    if len(values) == 1:
        values.append(jnp.zeros_like(values[0]))
    first, second = (values[1], values[0]) if flip else values
    return jnp.where(parity == 0, first, second)


def completed(geo, partial, sent, got, parity, below_top, full, halos):
    F, EX, EY, EZ, M = geo.F, geo.EX, geo.EY, geo.EZ, geo.M
    lanes = lane_iota((F, EZ))
    for f in range(3):
        for m in range(M):
            i, j = divmod(m, EY)
            v = partial[f, m]
            if f == 0 and i == 0 and got[0]:
                v = v + chosen(got[0], parity[0], lambda r: r[j], True)
            if f == 1 and j == 0 and got[1]:
                v = v + chosen(got[1], parity[1], lambda r: r[i], True)
            if f == 2 and got[2]:
                below = chosen(got[2], parity[2], lambda r: r[...], True)
                v = v + jnp.where(lanes == 0, moved(below, m, 0), 0.0)
            full[f, m] = v
    for a, n in ((0, EY), (1, EX)):
        for k in range(n):
            if got[a]:
                both = chosen(sent[a], parity[a], lambda r: r[k]) + chosen(got[a], parity[a], lambda r: r[k])
                halos[a][k] = both * below_top[a]
            else:
                halos[a][k] = jnp.zeros((F, EZ), f32)
    if got[2]:
        both = chosen(sent[2], parity[2], lambda r: r[...]) + chosen(got[2], parity[2], lambda r: r[...])
        halos[2][...] = both * below_top[2]
    else:
        halos[2][...] = jnp.zeros((F, EZ), f32)


def folded(total, value):
    v = value.reshape(value.shape[0] // 8, 8, value.shape[1]).sum(0)
    return v if total is None else total + v


def rows(ref, geo, f, m):
    return ref[pl.ds(f * geo.F * geo.M + m, geo.F, stride=geo.M), :]


def first_slabs(geo, trace, sx, sy, sz):
    F, EX, EY, EZ, M = geo.F, geo.EX, geo.EY, geo.EZ, geo.M
    lanes = lane_iota((F, EZ))
    for j in range(EY):
        sx[j] = rows(trace, geo, 0, j)
    for i in range(EX):
        sy[i] = rows(trace, geo, 1, i * EY)
    z = jnp.zeros((F, EZ), f32)
    for m in range(M):
        z = jnp.where(lanes == m, moved(rows(trace, geo, 2, m), 0, m), z)
    sz[...] = z


def take(refs, *sizes):
    refs = list(refs)
    out = []
    for s in sizes:
        if isinstance(s, (list, tuple)):
            group = []
            for n in s:
                group.append([refs.pop(0) for _ in range(n)])
            out.append(group)
        else:
            out.append([refs.pop(0) for _ in range(s)])
    assert not refs
    return out


def fetch(pairs, sems):
    copies = [pltpu.make_async_copy(src, dst, sems.at[k]) for k, (src, dst) in enumerate(pairs)]
    for c in copies:
        c.start()
    return copies


def kernel_prepare(geo, trace, load, diag_in, fine, coeff, schur, own, diag, weight, matrix, vload, vfine, vcoeff, vschur, sems):
    copies = fetch([(load, vload), (diag_in, diag), (fine, vfine), (coeff, vcoeff), (schur, vschur)], sems)
    for c in copies:
        c.wait()
    weight[...] = vfine[...].astype(f32) * vcoeff[...]
    n = 6 * geo.F
    matrix[:n], matrix[n:] = split(vschur[...])
    for f in range(3):
        for m in range(geo.M):
            own[f, m] = rows(vload, geo, f, m) - diag[f * geo.M + m:f * geo.M + m + 1] * rows(trace, geo, f, m)


def kernel_start(geo, n, trace, own, weight, schur, *refs):
    got, halos, (partial,), sends, (ghi, glo) = take(refs, n, 3, 1, n, 2)
    parity, _ = place()
    for a, k in ((0, geo.EY), (1, geo.EX)):
        for t in range(k):
            halos[a][t] = chosen(got[a], parity[a], lambda r: r[t]) if got[a] else jnp.zeros((geo.F, geo.EZ), f32)
    halos[2][...] = chosen(got[2], parity[2], lambda r: r[...]) if got[2] else jnp.zeros((geo.F, geo.EZ), f32)
    halo = (lambda j: halos[0][j], lambda i: halos[1][i], halos[2][...])
    y = gather_and_apply(geo, lambda f, m: rows(trace, geo, f, m), halo, schur, ghi, glo)
    spread(geo, y, weight[...], lambda f, m: own[f, m], -1.0, partial, sends, parity)


def accumulate(total, value):
    return value if total is None else total + value


def kernel_middle(geo, n, partial, diag, weight, schur, *refs):
    sent, got, (full,), halos, (image,), sends, (dots,), (ghi, glo) = take(refs, n, n, 1, 3, 1, n, 1, 2)
    F, EZ, M = geo.F, geo.EZ, geo.M
    parity, below_top = place()
    completed(geo, partial, sent, got, parity, below_top, full, halos)
    halo = (lambda j: halos[0][j], lambda i: halos[1][i], halos[2][...])
    y = gather_and_apply(geo, lambda f, m: full[f, m], halo, schur, ghi, glo)
    squares = energy = None
    for f in range(3):
        for m in range(M):
            vv = folded(None, full[f, m] * full[f, m])
            squares = accumulate(squares, vv)
            energy = accumulate(energy, vv * diag[f * M + m:f * M + m + 1])
    for m in range(M):
        part = None
        for s in range(6):
            at = (slice(s * F, (s + 1) * F), slice(m * EZ, (m + 1) * EZ))
            part = folded(part, (ghi[at].astype(f32) + glo[at].astype(f32)) * y[at])
        energy = energy + part * weight[m:m + 1]
    dots[0], dots[1] = squares, energy
    spread(geo, y, weight[...], lambda f, m: diag[f * M + m:f * M + m + 1] * full[f, m], 1.0, image, sends, parity)


def kernel_last(geo, n, partial, diag, weight, schur, dots, r, hxr, hyr, hzr, *refs):
    sent, got, (full,), halos, (message,), (ghi, glo) = take(refs, n, n, 1, 3, 1, 2)
    F, EX, EY, EZ, M = geo.F, geo.EX, geo.EY, geo.EZ, geo.M
    parity, below_top = place()
    completed(geo, partial, sent, got, parity, below_top, full, halos)
    along = None
    for f in range(3):
        for m in range(M):
            along = folded(along, r[f, m] * full[f, m])
    squares = jnp.sum(dots[0], keepdims=True)
    along = jnp.sum(along, keepdims=True)
    shift = jnp.where(squares > 0, jnp.clip(along / squares, -SHIFT_LIMIT, SHIFT_LIMIT), 0.0)
    halo = (lambda j: halos[0][j] - shift * hxr[j], lambda i: halos[1][i] - shift * hyr[i], halos[2][...] - shift * hzr[...])
    y = gather_and_apply(geo, lambda f, m: full[f, m] - shift * r[f, m], halo, schur, ghi, glo)
    rp = pp = erp = epp = None
    for f in range(3):
        for m in range(M):
            v = r[f, m]
            p = full[f, m] - shift * v
            d = diag[f * M + m:f * M + m + 1]
            a, b = folded(None, v * p), folded(None, p * p)
            rp, pp = accumulate(rp, a), accumulate(pp, b)
            erp, epp = accumulate(erp, a * d), accumulate(epp, b * d)
    lanes = lane_iota((F, EZ))
    for m in range(M):
        i, j = divmod(m, EY)
        blocks = [
            r[0, m], r[0, m + EY] if i + 1 < EX else hxr[j],
            r[1, m], r[1, m + 1] if j + 1 < EY else hyr[i],
            r[2, m], jnp.where(lanes == EZ - 1, moved(hzr[...], m, EZ - 1), moved(r[2, m], 1, 0)),
        ]
        one = two = None
        for s, block in enumerate(blocks):
            at = (slice(s * F, (s + 1) * F), slice(m * EZ, (m + 1) * EZ))
            one = folded(one, block * y[at])
            two = folded(two, (ghi[at].astype(f32) + glo[at].astype(f32)) * y[at])
        erp = erp + one * weight[m:m + 1]
        epp = epp + two * weight[m:m + 1]
    lane = lane_iota((1, EZ))
    line = jnp.where(lane == 0, shift, jnp.where(lane == 1, squares, 0.0))
    for k, v in enumerate((rp, pp, dots[1], erp, epp)):
        line = jnp.where(lane == k + 2, jnp.sum(v, keepdims=True), line)
    message[...] = jnp.broadcast_to(line, message.shape)


def step_sizes(rows_of_devices):
    lanes = lane_iota(rows_of_devices.shape)
    theta, rr, rp, pp, err, erp, epp = [jnp.sum(jnp.where(lanes == k, rows_of_devices, 0.0), 1, keepdims=True) for k in range(7)]

    def total(v):
        return jnp.sum(v, 0, keepdims=True)

    old = total(rr)
    alpha = old / total(err)
    u = 1.0 - alpha * theta
    new = total(u * u * rr - 2.0 * u * alpha * rp + alpha * alpha * pp)
    beta = new / old
    c = u + beta
    energy = total(c * c * err - 2.0 * c * alpha * erp + alpha * alpha * epp)
    second = jnp.where(energy > 0, new / energy, 0.0)
    return alpha + second * (1.0 + beta), -alpha * second


def kernel_volume(geo, fields, fine, operator, base, plain, vfields, vfine, voperator, vbase, sems):
    M, EZ = geo.M, geo.EZ
    dofs = operator.shape[0]
    for c in fetch([(fields, vfields), (fine, vfine), (operator, voperator)], sems):
        c.wait()
    plain[...] = vfields[...].astype(f32)
    nodal = [plain[pl.ds(m, dofs, stride=M), :] for m in range(M)]
    volume = jnp.dot(voperator[...], jnp.concatenate([v.astype(bf16) for v in nodal], 1), preferred_element_type=f32)
    coarse = 1.0 - vfine[...].astype(f32)
    for m in range(M):
        vbase[m] = nodal[m] + (TIME_STEP * coarse[m:m + 1]) * volume[:, m * EZ:(m + 1) * EZ]
    copy = pltpu.make_async_copy(vbase, base, sems.at[0])
    copy.start()
    copy.wait()


def kernel_finish(geo, message, trace, base, fine, lift, r, q, *refs):
    (hx, hy, hz), (hxr, hyr, hzr), (hxq, hyq, hzq), (fields_new, trace_new), (g, plain, vbase, sems) = take(refs, 3, 3, 3, 2, 4)
    F, EX, EY, EZ, M = geo.F, geo.EX, geo.EY, geo.EZ, geo.M
    copy = pltpu.make_async_copy(base, vbase, sems.at[0])
    copy.start()
    lanes = lane_iota((F, EZ))
    cr, cq = step_sizes(message[...])
    flag = fine[...].astype(f32)
    z_step = cr * hzr[...] + cq * hzq[...]
    for m in range(M):
        i, j = divmod(m, EY)
        mark = flag[m:m + 1]

        def old_step(f, k):
            return rows(trace, geo, f, k), cr * r[f, k] + cq * q[f, k]

        ox, sx = old_step(0, m)
        oy, sy = old_step(1, m)
        oz, sz = old_step(2, m)
        for f, (o, s) in enumerate(((ox, sx), (oy, sy), (oz, sz))):
            trace_new[pl.ds(f * F * M + m, F, stride=M), :] = o + s
        up_x = old_step(0, m + EY) if i + 1 < EX else (hx[j], cr * hxr[j] + cq * hxq[j])
        up_y = old_step(1, m + 1) if j + 1 < EY else (hy[i], cr * hyr[i] + cq * hyq[i])
        up_z = tuple(jnp.where(lanes == EZ - 1, moved(h, m, EZ - 1), moved(v, 1, 0)) for h, v in ((hz[...], oz), (z_step, sz)))
        for s, (o, step) in enumerate(((ox, sx), up_x, (oy, sy), up_y, (oz, sz), up_z)):
            g[s * F:(s + 1) * F, m * EZ:(m + 1) * EZ] = (o + mark * step).astype(bf16)
    lifted = jnp.dot(lift[...], g[...], preferred_element_type=f32)
    dofs = lift.shape[0]
    copy.wait()
    for m in range(M):
        plain[pl.ds(m, dofs, stride=M), :] = vbase[m] + TIME_STEP * lifted[:, m * EZ:(m + 1) * EZ]
    fields_new[...] = plain[...].astype(bf16)


VMEM, HBM = pltpu.MemorySpace.VMEM, pltpu.MemorySpace.HBM


def call(kernel, outs, args, scratch, flops, hbm_args=(), hbm_outs=()):
    def specs(count, in_hbm):
        return [pl.BlockSpec(memory_space=HBM if k in in_hbm else VMEM) for k in range(count)]

    return pl.pallas_call(
        kernel,
        out_shape=[jax.ShapeDtypeStruct(s, d) for s, d in outs],
        in_specs=specs(len(args), hbm_args),
        out_specs=specs(len(outs), hbm_outs),
        scratch_shapes=scratch,
        cost_estimate=pl.CostEstimate(flops=flops, bytes_accessed=1 << 20, transcendentals=0),
        compiler_params=pltpu.CompilerParams(vmem_limit_bytes=VMEM_GRANT),
    )(*args)


def flat(groups):
    return [v for group in groups for v in group if v is not None]


def like(array):
    return pltpu.VMEM(array.shape, array.dtype)


def body(fields, trace_old, face_load, face_diag, fine_flag, coeff, volume_op, lift_op, schur_op):
    _, F, EX, EY, EZ = trace_old.shape
    geo = Geometry(F, EX, EY, EZ)
    M, dofs, N = geo.M, fields.shape[0], 6 * F
    devices = 1
    for a in AXES:
        devices *= lax.axis_size(a)
    n = counts()
    trace = trace_old.reshape(3 * F * M, EZ)
    load = face_load.reshape(3 * F * M, EZ)
    diag_in = face_diag.reshape(3 * M, EZ)
    fine = fine_flag.reshape(M, EZ)
    scale = coeff.reshape(M, EZ)
    nodal = fields.reshape(dofs * M, EZ)
    slab = [(EY, F, EZ), (EX, F, EZ), (F, EZ)]
    full = (3, M, F, EZ)
    halo_outs = [(s, f32) for s in slab]
    send_outs = [(s, f32) for s, k in zip(slab, n) for _ in range(k)]
    halves = [pltpu.VMEM((N, M * EZ), bf16)] * 2
    flops = 2 * 3 * N * N * M * EZ
    dma = pltpu.SemaphoreType.DMA

    def grouped(values):
        values = list(values)
        return [[values.pop(0) for _ in range(k)] for k in n]

    slabs = call(functools.partial(first_slabs, geo), halo_outs, [trace], [], 1 << 20)
    got = exchange([[s, s] for s in slabs])
    own, diag, weight, schur = call(
        functools.partial(kernel_prepare, geo), [(full, f32), ((3 * M, EZ), f32), ((M, EZ), f32), ((2 * N, N), bf16)],
        [trace, load, diag_in, fine, scale, schur_op], [like(load), like(fine), like(scale), like(schur_op), dma((5,))],
        flops, hbm_args=(1, 2, 3, 4, 5))
    out = call(functools.partial(kernel_start, geo, n), halo_outs + [(full, f32)] + send_outs,
               [trace, own, weight, schur] + flat(got), halves, flops)
    halo_old, partial, sent = out[:3], out[3], grouped(out[4:])
    got = exchange(sent)
    out = call(functools.partial(kernel_middle, geo, n), [(full, f32)] + halo_outs + [(full, f32)] + send_outs + [((2, 8, EZ), f32)],
               [partial, diag, weight, schur] + flat(sent) + flat(got), halves, flops)
    r, halo_r, partial, sent, dots = out[0], out[1:4], out[4], grouped(out[5:-1]), out[-1]
    got = exchange(sent)
    out = call(functools.partial(kernel_last, geo, n), [(full, f32)] + halo_outs + [((devices, EZ), f32)],
               [partial, diag, weight, schur, dots, r, *halo_r] + flat(sent) + flat(got), halves, flops)
    q, halo_q, message = out[0], out[1:4], out[4]
    message = lax.all_to_all(message, AXES, 0, 0, tiled=True)
    base = call(functools.partial(kernel_volume, geo), [((M, dofs, EZ), f32)], [nodal, fine, volume_op],
                [pltpu.VMEM((dofs * M, EZ), f32), like(nodal), like(fine), like(volume_op), pltpu.VMEM((M, dofs, EZ), f32), dma((3,))],
                2 * dofs * dofs * M * EZ, hbm_args=(0, 1, 2), hbm_outs=(0,))[0]
    fields_new, trace_new = call(
        functools.partial(kernel_finish, geo), [((dofs * M, EZ), bf16), ((3 * F * M, EZ), f32)],
        [message, trace, base, fine, lift_op, r, q, *halo_old, *halo_r, *halo_q],
        [pltpu.VMEM((N, M * EZ), bf16), pltpu.VMEM((dofs * M, EZ), f32), pltpu.VMEM((M, dofs, EZ), f32), dma((1,))],
        2 * dofs * N * M * EZ, hbm_args=(2,))
    return fields_new.reshape(fields.shape), trace_new.reshape(trace_old.shape)


def solution(mesh):
    placed = (
        P(None, *AXES), P(None, None, *AXES), P(None, None, *AXES), P(None, *AXES), P(*AXES), P(*AXES), P(), P(), P(),
    )
    return jax.shard_map(body, mesh=mesh, in_specs=placed, out_specs=(P(None, *AXES), P(None, None, *AXES)), check_vma=False)
```

```python
import functools

import jax
import jax.numpy as jnp
from jax import lax
from jax.experimental import pallas as pl
from jax.experimental.pallas import tpu as pltpu
from jax.sharding import PartitionSpec as P

AXES = ("gx", "gy", "gz")
TIME_STEP = 0.25
SHIFT_LIMIT = 1e4
PARTS = 4
STRIDE = 8
VMEM_GRANT = 12 * 1024 * 1024
f32, bf16 = jnp.float32, jnp.bfloat16


def pairs(axis, odd):
    size = lax.axis_size(axis)
    route = []
    for i in range(odd, size - 1, 2):
        route += [(i, i + 1), (i + 1, i)]
    return route


def exchange(axes, sends):
    return [[lax.ppermute(v, axis, pairs(axis, odd)) for odd, v in enumerate(s) if pairs(axis, odd)] for axis, s in zip(axes, sends)]


def counts():
    return [sum(bool(pairs(axis, odd)) for odd in (0, 1)) for axis in AXES]


def lane_iota(shape):
    return lax.broadcasted_iota(jnp.int32, shape, len(shape) - 1)


def moved(value, source, target):
    width = value.shape[-1]
    shift = (target - source) % width
    return pltpu.roll(value, shift, value.ndim - 1) if shift else value


def place():
    index = [lax.axis_index(a) for a in AXES]
    parity = [lax.rem(i, 2) for i in index]
    below_top = [(i < lax.axis_size(a) - 1).astype(f32) for i, a in zip(index, AXES)]
    return parity, below_top


def split(value):
    high = value.astype(bf16)
    return high, (value - high.astype(f32)).astype(bf16)


class Geometry:
    def __init__(self, F, EX, EY, EZ):
        self.F, self.EX, self.EY, self.EZ = F, EX, EY, EZ
        self.M = EX * EY


def at_rows(geo, s, m):
    return slice(s * geo.F, (s + 1) * geo.F), slice(m * geo.EZ, (m + 1) * geo.EZ)


def lanes_of(geo):
    lane = lane_iota((geo.F, geo.EZ))
    return lane, lane % STRIDE, lane // (STRIDE * geo.EY), (lane // STRIDE) % geo.EY


def z_above(geo, z_own, z_pack, m):
    lane = lane_iota((geo.F, geo.EZ))
    return jnp.where(lane == geo.EZ - 1, moved(z_pack, m * STRIDE + 2, geo.EZ - 1), moved(z_own, 1, 0))


def gather_and_apply(geo, own, halo, schur, ghi, glo, wide=None):
    F, EX, EY, EZ, M = geo.F, geo.EX, geo.EY, geo.EZ, geo.M
    hx, hy, hz = halo

    def put(m, blocks):
        for s, block in enumerate(blocks):
            high, low = split(block)
            ghi[at_rows(geo, s, m)] = high
            glo[at_rows(geo, s, m)] = low

    bottom = jnp.zeros((F, EZ), f32)
    lane, column, at_i, at_j = lanes_of(geo)
    for m in range(M):
        i, j = divmod(m, EY)
        z_own = own(2, m)
        put(m, [
            own(0, m), own(0, m + EY) if i + 1 < EX else hx(j),
            own(1, m), own(1, m + 1) if j + 1 < EY else hy(i),
            z_own, z_above(geo, z_own, hz, m),
        ])
        if wide:
            bottom = jnp.where(lane == m * STRIDE + 1, moved(z_own, 0, m * STRIDE + 1), bottom)
    if wide:
        x, y, hx_pack, hy_pack = wide
        put(M, [
            x, jnp.where(at_i == EX - 1, moved(hx_pack, 0, (EX - 1) * EY * STRIDE), moved(x, EY * STRIDE, 0)),
            y, jnp.where(at_j == EY - 1, moved(hy_pack, 0, (EY - 1) * STRIDE), moved(y, STRIDE, 0)),
            hz, jnp.where(column == 1, bottom, moved(hz, 1, 0)),
        ])
    n = 6 * F
    both = jnp.dot(schur[...], ghi[...], preferred_element_type=f32)
    return both[:n] + (both[n:] + jnp.dot(schur[:n], glo[...], preferred_element_type=f32))


def spread(geo, y, weight, own_term, sign, out, sends, parity, weight_pack, own_pack, pack_out):
    F, EX, EY, EZ, M = geo.F, geo.EX, geo.EY, geo.EZ, geo.M
    lane, column, at_i, at_j = lanes_of(geo)
    wrow = [weight[m:m + 1] * sign for m in range(M)] + [weight_pack * sign]

    def block(s, m):
        return y[at_rows(geo, s, m)] * wrow[m]

    low = {}
    below = block(5, M)
    top = jnp.zeros((F, EZ), f32)
    for m in range(M):
        i, j = divmod(m, EY)
        vx = own_term(0, m) + block(0, m)
        if i > 0:
            vx = vx + block(1, m - EY)
        else:
            low[0, j] = vx
        out[0, m] = vx
        vy = own_term(1, m) + block(2, m)
        if j > 0:
            vy = vy + block(3, m - 1)
        else:
            low[1, i] = vy
        out[1, m] = vy
        up = block(5, m)
        out[2, m] = own_term(2, m) + block(4, m) + jnp.where(lane == 0, moved(below, m * STRIDE + 1, 0), moved(up, 0, 1))
        top = jnp.where(lane == m * STRIDE + 2, moved(up, EZ - 1, m * STRIDE + 2), top)
    shared = [
        [(low[0, j], block(1, (EX - 1) * EY + j)) for j in range(EY)],
        [(low[1, i], block(3, i * EY + EY - 1)) for i in range(EX)],
    ]
    pack_out[2][...] = own_pack(2) + block(4, M) + jnp.where(column == 2, top, moved(below, 0, 1))
    if 0 in pack_out:
        up = block(1, M)
        v = own_pack(0) + block(0, M)
        pack_out[0][...] = v + jnp.where(at_i > 0, moved(up, 0, EY * STRIDE), 0.0)
        shared[0].append((v, moved(up, (EX - 1) * EY * STRIDE, 0)))
        up = block(3, M)
        v = own_pack(1) + block(2, M)
        pack_out[1][...] = v + jnp.where(at_j > 0, moved(up, 0, STRIDE), 0.0)
        shared[1].append((v, moved(up, (EY - 1) * STRIDE, 0)))
    for a in (0, 1):
        for odd, ref in enumerate(sends[a]):
            for k, (bottom, high) in enumerate(shared[a]):
                ref[k] = jnp.where(parity[a] == odd, high, bottom)


def chosen(refs, parity, read, flip=False):
    values = [read(r) for r in refs]
    if not values:
        return None
    if len(values) == 1:
        values.append(jnp.zeros_like(values[0]))
    first, second = (values[1], values[0]) if flip else values
    return jnp.where(parity == 0, first, second)


def completed(geo, partial, sent, got, parity, below_top, full, halos):
    F, EX, EY, EZ, M = geo.F, geo.EX, geo.EY, geo.EZ, geo.M
    for f in range(3):
        for m in range(M):
            i, j = divmod(m, EY)
            v = partial[f, m]
            if f == 0 and i == 0 and got[0]:
                v = v + chosen(got[0], parity[0], lambda r: r[j], True)
            if f == 1 and j == 0 and got[1]:
                v = v + chosen(got[1], parity[1], lambda r: r[i], True)
            full[f, m] = v
    for a, n in ((0, EY), (1, EX)):
        for k in range(n):
            halos[a][k] = both_sides(geo, sent[a], got[a], parity[a], below_top[a], k)


def both_sides(geo, sent, got, parity, below_top, k):
    if not got:
        return jnp.zeros((geo.F, geo.EZ), f32)
    return (chosen(sent, parity, lambda r: r[k]) + chosen(got, parity, lambda r: r[k])) * below_top


def folded(total, value):
    v = value.reshape(value.shape[0] // 8, 8, value.shape[1]).sum(0)
    return v if total is None else total + v


def rows(ref, geo, f, m):
    return ref[pl.ds(f * geo.F * geo.M + m, geo.F, stride=geo.M), :]


def kernel_pack(geo, trace, load, diag, fine, coeff, pack, vtrace, vload, vdiag, vfine, vcoeff, sems):
    F, EZ, M = geo.F, geo.EZ, geo.M
    for c in fetch([(trace, vtrace), (load, vload), (diag, vdiag), (fine, vfine), (coeff, vcoeff)], sems):
        c.wait()
    half = EZ // 2

    def packed(parts):
        shape = parts[0].shape
        lane = lane_iota(shape)
        out = jnp.zeros(shape, f32)
        for m, part in enumerate(parts):
            start = (m // M) * half + (m % M) * STRIDE
            out = jnp.where((lane >= start) & (lane < start + 5), moved(part, 0, start + 2), out)
        return out

    for f in range(3):
        pack[f * F:(f + 1) * F] = packed([rows(v, geo, f, m) for v in (vtrace, vload) for m in range(M)])
    weight = vfine[...].astype(f32) * vcoeff[...]
    lines = [packed([vdiag[f * M + m:f * M + m + 1] for m in range(M)]) for f in range(3)]
    lines.append(packed([weight[m:m + 1] for m in range(M)]))
    for k in range(8):
        pack[3 * F + k:3 * F + k + 1] = lines[min(k, 3)]


def kernel_wide(geo, n, trace, _, *refs):
    got, (trace_pack, own_pack, lines, sx, sy) = take(refs, n[2:], 5)
    F, EX, EY, EZ = geo.F, geo.EX, geo.EY, geo.EZ
    parity, _ = place()
    lane = lane_iota((F, EZ))

    def mixed(rows_at):
        if not got[0]:
            return jnp.zeros((F, EZ), f32)[:rows_at.stop - rows_at.start]
        below = chosen(got[0], parity[2], lambda r: r[rows_at], True)
        above = chosen(got[0], parity[2], lambda r: r[rows_at])
        return jnp.where(lane[:below.shape[0]] % STRIDE < 2, below, above)

    lines[...] = mixed(slice(3 * F, 3 * F + 8))
    for f in range(3):
        v = mixed(slice(f * F, (f + 1) * F))
        old = jnp.where(lane < EZ // 2, v, 0.0)
        load = jnp.where(lane < EZ // 2, moved(v, EZ // 2, 0), 0.0)
        trace_pack[f] = old
        own_pack[f] = load - lines[f:f + 1] * old
        if f == 0:
            for j in range(EY):
                sx[j] = rows(trace, geo, 0, j)
            sx[EY] = old
        if f == 1:
            for i in range(EX):
                sy[i] = rows(trace, geo, 1, i * EY)
            sy[EX] = old


def take(refs, *sizes):
    refs = list(refs)
    out = []
    for s in sizes:
        if isinstance(s, (list, tuple)):
            group = []
            for n in s:
                group.append([refs.pop(0) for _ in range(n)])
            out.append(group)
        else:
            out.append([refs.pop(0) for _ in range(s)])
    assert not refs
    return out


def fetch(pairs, sems):
    copies = [pltpu.make_async_copy(src, dst, sems.at[k]) for k, (src, dst) in enumerate(pairs)]
    for c in copies:
        c.start()
    return copies


def kernel_prepare(geo, trace, load, diag_in, fine, coeff, schur, own, diag, weight, matrix, vload, vfine, vcoeff, vschur, sems):
    copies = fetch([(load, vload), (diag_in, diag), (fine, vfine), (coeff, vcoeff), (schur, vschur)], sems)
    for c in copies:
        c.wait()
    weight[...] = vfine[...].astype(f32) * vcoeff[...]
    n = 6 * geo.F
    matrix[:n], matrix[n:] = split(vschur[...])
    for f in range(3):
        for m in range(geo.M):
            own[f, m] = rows(vload, geo, f, m) - diag[f * geo.M + m:f * geo.M + m + 1] * rows(trace, geo, f, m)


def kernel_start(geo, n, trace, own, weight, schur, trace_pack, own_pack, lines, *refs):
    got, halos, (partial, partial_pack), sends, (ghi, glo) = take(refs, n[:2], 2, 2, n[:2], 2)
    F, EX, EY, EZ = geo.F, geo.EX, geo.EY, geo.EZ
    parity, _ = place()

    def above(a, k):
        return chosen(got[a], parity[a], lambda r: r[k]) if got[a] else jnp.zeros((F, EZ), f32)

    for a, count in ((0, EY), (1, EX)):
        for k in range(count):
            halos[a][k] = above(a, k)
    halo = (lambda j: halos[0][j], lambda i: halos[1][i], trace_pack[2])
    wide = (trace_pack[0], trace_pack[1], above(0, EY), above(1, EX))
    y = gather_and_apply(geo, lambda f, m: rows(trace, geo, f, m), halo, schur, ghi, glo, wide)
    spread(geo, y, weight[...], lambda f, m: own[f, m], -1.0, partial, sends, parity,
           lines[3:4], lambda f: own_pack[f], {f: partial_pack.at[f] for f in range(3)})


def accumulate(total, value):
    return value if total is None else total + value


def kernel_middle(geo, n, partial, partial_pack, diag, weight, schur, lines, *refs):
    sent, got, (full, full_z), halos, (image, image_z), sends, (dots,), (ghi, glo) = take(refs, n[:2], n[:2], 2, 2, 2, n[:2], 1, 2)
    F, EX, EY, EZ, M = geo.F, geo.EX, geo.EY, geo.EZ, geo.M
    parity, below_top = place()
    completed(geo, partial, sent, got, parity, below_top, full, halos)
    lane, column, at_i, at_j = lanes_of(geo)
    packs = []
    for a, edge, count in ((0, at_i == 0, EY), (1, at_j == 0, EX)):
        v = partial_pack[a]
        if got[a]:
            v = v + jnp.where(edge, chosen(got[a], parity[a], lambda r: r[count], True), 0.0)
        packs.append(v)
    wide = (*packs, both_sides(geo, sent[0], got[0], parity[0], below_top[0], EY), both_sides(geo, sent[1], got[1], parity[1], below_top[1], EX))
    full_z[...] = jnp.where(column < 2, partial_pack[2], partial_pack[2] * below_top[2])
    halo = (lambda j: halos[0][j], lambda i: halos[1][i], full_z[...])
    y = gather_and_apply(geo, lambda f, m: full[f, m], halo, schur, ghi, glo, wide)
    squares = energy = None
    for f in range(3):
        for m in range(M):
            vv = folded(None, full[f, m] * full[f, m])
            squares = accumulate(squares, vv)
            energy = accumulate(energy, vv * diag[f * M + m:f * M + m + 1])
    for m in range(M):
        part = None
        for s in range(6):
            at = at_rows(geo, s, m)
            part = folded(part, (ghi[at].astype(f32) + glo[at].astype(f32)) * y[at])
        energy = energy + part * weight[m:m + 1]
    dots[0], dots[1] = squares, energy
    spread(geo, y, weight[...], lambda f, m: diag[f * M + m:f * M + m + 1] * full[f, m], 1.0, image, sends, parity,
           lines[3:4], lambda f: lines[f:f + 1] * full_z[...], {2: image_z})
    image_z[...] = image_z[...] * below_top[2]


def kernel_last(geo, n, partial, image_z, diag, weight, schur, dots, r, hxr, hyr, hzr, *refs):
    sent, got, (full,), halos, (message,), (ghi, glo) = take(refs, n[:2], n[:2], 1, 2, 1, 2)
    F, EX, EY, EZ, M = geo.F, geo.EX, geo.EY, geo.EZ, geo.M
    parity, below_top = place()
    completed(geo, partial, sent, got, parity, below_top, full, halos)
    along = None
    for f in range(3):
        for m in range(M):
            along = folded(along, r[f, m] * full[f, m])
    squares = jnp.sum(dots[0], keepdims=True)
    along = jnp.sum(along, keepdims=True)
    shift = jnp.where(squares > 0, jnp.clip(along / squares, -SHIFT_LIMIT, SHIFT_LIMIT), 0.0)
    halo = (lambda j: halos[0][j] - shift * hxr[j], lambda i: halos[1][i] - shift * hyr[i], image_z[...] - shift * hzr[...])
    y = gather_and_apply(geo, lambda f, m: full[f, m] - shift * r[f, m], halo, schur, ghi, glo)
    rp = pp = erp = epp = None
    for f in range(3):
        for m in range(M):
            v = r[f, m]
            p = full[f, m] - shift * v
            d = diag[f * M + m:f * M + m + 1]
            a, b = folded(None, v * p), folded(None, p * p)
            rp, pp = accumulate(rp, a), accumulate(pp, b)
            erp, epp = accumulate(erp, a * d), accumulate(epp, b * d)
    for m in range(M):
        i, j = divmod(m, EY)
        blocks = [
            r[0, m], r[0, m + EY] if i + 1 < EX else hxr[j],
            r[1, m], r[1, m + 1] if j + 1 < EY else hyr[i],
            r[2, m], z_above(geo, r[2, m], hzr[...], m),
        ]
        one = two = None
        for s, block in enumerate(blocks):
            at = at_rows(geo, s, m)
            one = folded(one, block * y[at])
            two = folded(two, (ghi[at].astype(f32) + glo[at].astype(f32)) * y[at])
        erp = erp + one * weight[m:m + 1]
        epp = epp + two * weight[m:m + 1]
    lane = lane_iota((1, EZ))
    line = jnp.where(lane == 0, shift, jnp.where(lane == 1, squares, 0.0))
    for k, v in enumerate((rp, pp, dots[1], erp, epp)):
        line = jnp.where(lane == k + 2, jnp.sum(v, keepdims=True), line)
    message[...] = jnp.broadcast_to(line, message.shape)


def step_sizes(rows_of_devices):
    lanes = lane_iota(rows_of_devices.shape)
    theta, rr, rp, pp, err, erp, epp = [jnp.sum(jnp.where(lanes == k, rows_of_devices, 0.0), 1, keepdims=True) for k in range(7)]

    def total(v):
        return jnp.sum(v, 0, keepdims=True)

    old = total(rr)
    alpha = old / total(err)
    u = 1.0 - alpha * theta
    new = total(u * u * rr - 2.0 * u * alpha * rp + alpha * alpha * pp)
    beta = new / old
    c = u + beta
    energy = total(c * c * err - 2.0 * c * alpha * erp + alpha * alpha * epp)
    second = jnp.where(energy > 0, new / energy, 0.0)
    return alpha + second * (1.0 + beta), -alpha * second


def kernel_volume(geo, fields, fine, operator, base, plain, vfields, vfine, voperator, sems):
    M, EZ = geo.M, geo.EZ
    dofs = operator.shape[0]
    for c in fetch([(fields, vfields), (fine, vfine), (operator, voperator)], sems):
        c.wait()
    plain[...] = vfields[...].astype(f32)
    nodal = [plain[pl.ds(m, dofs, stride=M), :] for m in range(M)]
    volume = jnp.dot(voperator[...], jnp.concatenate([v.astype(bf16) for v in nodal], 1), preferred_element_type=f32)
    coarse = 1.0 - vfine[...].astype(f32)
    for m in range(M):
        base[m] = nodal[m] + (TIME_STEP * coarse[m:m + 1]) * volume[:, m * EZ:(m + 1) * EZ]


def kernel_finish(geo, message, trace, base, fine, lift, r, q, *refs):
    (hx, hy, hz), (hxr, hyr, hzr), (hxq, hyq, hzq), (fields_out, trace_out), (g, plain, fields_new, trace_new, sems) = take(refs, 3, 3, 3, 2, 5)
    F, EX, EY, EZ, M = geo.F, geo.EX, geo.EY, geo.EZ, geo.M
    cr, cq = step_sizes(message[...])
    flag = fine[...].astype(f32)
    z_step = cr * hzr[...] + cq * hzq[...]
    for m in range(M):
        i, j = divmod(m, EY)
        mark = flag[m:m + 1]

        def old_step(f, k):
            return rows(trace, geo, f, k), cr * r[f, k] + cq * q[f, k]

        ox, sx = old_step(0, m)
        oy, sy = old_step(1, m)
        oz, sz = old_step(2, m)
        for f, (o, s) in enumerate(((ox, sx), (oy, sy), (oz, sz))):
            trace_new[pl.ds(f * F * M + m, F, stride=M), :] = o + s
        up_x = old_step(0, m + EY) if i + 1 < EX else (hx[j], cr * hxr[j] + cq * hxq[j])
        up_y = old_step(1, m + 1) if j + 1 < EY else (hy[i], cr * hyr[i] + cq * hyq[i])
        up_z = (z_above(geo, oz, hz[2], m), z_above(geo, sz, z_step, m))
        for s, (o, step) in enumerate(((ox, sx), up_x, (oy, sy), up_y, (oz, sz), up_z)):
            g[s * F:(s + 1) * F, m * EZ:(m + 1) * EZ] = (o + mark * step).astype(bf16)
    copies = [pltpu.make_async_copy(trace_new, trace_out, sems.at[0])]
    copies[0].start()
    dofs = lift.shape[0]
    part = dofs // PARTS
    for k in range(PARTS):
        lifted = jnp.dot(lift[k * part:(k + 1) * part], g[...], preferred_element_type=f32)
        for m in range(M):
            plain[pl.ds(k * part * M + m, part, stride=M), :] = base[m, k * part:(k + 1) * part] + TIME_STEP * lifted[:, m * EZ:(m + 1) * EZ]
        some = pl.ds(k * part * M, part * M)
        fields_new[some] = plain[some].astype(bf16)
        copies.append(pltpu.make_async_copy(fields_new.at[some], fields_out.at[some], sems.at[k + 1]))
        copies[-1].start()
    for c in copies:
        c.wait()


VMEM, HBM = pltpu.MemorySpace.VMEM, pltpu.MemorySpace.HBM


def call(kernel, outs, args, scratch, flops, hbm_args=(), hbm_outs=()):
    def specs(count, in_hbm):
        return [pl.BlockSpec(memory_space=HBM if k in in_hbm else VMEM) for k in range(count)]

    args = [pltpu.with_memory_space_constraint(v, HBM) if k in hbm_args else v for k, v in enumerate(args)]
    return pl.pallas_call(
        kernel,
        out_shape=[(HBM if k in hbm_outs else jax.ShapeDtypeStruct)(s, d) for k, (s, d) in enumerate(outs)],
        in_specs=specs(len(args), hbm_args),
        out_specs=specs(len(outs), hbm_outs),
        scratch_shapes=scratch,
        cost_estimate=pl.CostEstimate(flops=flops, bytes_accessed=1 << 20, transcendentals=0),
        compiler_params=pltpu.CompilerParams(vmem_limit_bytes=VMEM_GRANT),
    )(*args)


def flat(groups):
    return [v for group in groups for v in group if v is not None]


def like(array):
    return pltpu.VMEM(array.shape, array.dtype)


def body(fields, trace_old, face_load, face_diag, fine_flag, coeff, volume_op, lift_op, schur_op):
    _, F, EX, EY, EZ = trace_old.shape
    geo = Geometry(F, EX, EY, EZ)
    M, dofs, N = geo.M, fields.shape[0], 6 * F
    devices = 1
    for a in AXES:
        devices *= lax.axis_size(a)
    n = counts()
    trace = trace_old.reshape(3 * F * M, EZ)
    load = face_load.reshape(3 * F * M, EZ)
    diag_in = face_diag.reshape(3 * M, EZ)
    fine = fine_flag.reshape(M, EZ)
    scale = coeff.reshape(M, EZ)
    nodal = fields.reshape(dofs * M, EZ)
    slab = [(EY, F, EZ), (EX, F, EZ)]
    slab_wide = [(EY + 1, F, EZ), (EX + 1, F, EZ)]
    full, pack, line = (3, M, F, EZ), (3, F, EZ), (8, EZ)
    halo_outs = [(s, f32) for s in slab]
    flops = 2 * 3 * N * N * M * EZ
    dma = pltpu.SemaphoreType.DMA

    def halves(blocks):
        return [pltpu.VMEM((N, blocks * EZ), bf16)] * 2

    def send_outs(shapes):
        return [(s, f32) for s, k in zip(shapes, n) for _ in range(k)]

    def grouped(values):
        values = list(values)
        return [[values.pop(0) for _ in range(k)] for k in n[:2]]

    packed, held = call(functools.partial(kernel_pack, geo), [((3 * F + 8, EZ), f32), (trace.shape, f32)], [trace, load, diag_in, fine, scale],
                        [like(load), like(diag_in), like(fine), like(scale), dma((5,))], 1 << 20, hbm_args=range(5))
    got = exchange(AXES[2:], [[packed, packed]])
    own, diag, weight, schur = call(
        functools.partial(kernel_prepare, geo), [(full, f32), ((3 * M, EZ), f32), ((M, EZ), f32), ((2 * N, N), bf16)],
        [held, load, diag_in, fine, scale, schur_op], [like(load), like(fine), like(scale), like(schur_op), dma((5,))],
        flops, hbm_args=(1, 2, 3, 4, 5))
    trace_pack, own_pack, lines, sx, sy = call(
        functools.partial(kernel_wide, geo, n), [(pack, f32), (pack, f32), (line, f32)] + [(s, f32) for s in slab_wide],
        [held, weight] + flat(got), [], 1 << 20)
    got = exchange(AXES[:2], [[sx, sx], [sy, sy]])
    out = call(functools.partial(kernel_start, geo, n), halo_outs + [(full, f32), (pack, f32)] + send_outs(slab_wide),
               [held, own, weight, schur, trace_pack, own_pack, lines] + flat(got), halves(M + 1), flops)
    halo_old, partial, partial_pack, sent = [*out[:2], trace_pack], out[2], out[3], grouped(out[4:])
    got = exchange(AXES[:2], sent)
    out = call(functools.partial(kernel_middle, geo, n),
               [(full, f32), ((F, EZ), f32)] + halo_outs + [(full, f32), ((F, EZ), f32)] + send_outs(slab) + [((2, 8, EZ), f32)],
               [partial, partial_pack, diag, weight, schur, lines] + flat(sent) + flat(got), halves(M + 1), flops)
    r, r_z, partial, image_z, sent, dots = out[0], out[1], out[4], out[5], grouped(out[6:-1]), out[-1]
    halo_r = [*out[2:4], r_z]
    got = exchange(AXES[:2], sent)
    out = call(functools.partial(kernel_last, geo, n), [(full, f32)] + halo_outs + [((devices, EZ), f32)],
               [partial, image_z, diag, weight, schur, dots, r, *halo_r] + flat(sent) + flat(got), halves(M), flops)
    q, halo_q, message = out[0], [*out[1:3], image_z], out[3]
    message = lax.all_to_all(message, AXES, 0, 0, tiled=True)
    base = call(functools.partial(kernel_volume, geo), [((M, dofs, EZ), f32)], [nodal, fine, volume_op],
                [pltpu.VMEM((dofs * M, EZ), f32), like(nodal), like(fine), like(volume_op), dma((3,))],
                2 * dofs * dofs * M * EZ, hbm_args=(0, 1, 2))[0]
    fields_new, trace_new = call(
        functools.partial(kernel_finish, geo), [((dofs * M, EZ), bf16), ((3 * F * M, EZ), f32)],
        [message, trace, base, fine, lift_op, r, q, *halo_old, *halo_r, *halo_q],
        [pltpu.VMEM((N, M * EZ), bf16), pltpu.VMEM((dofs * M, EZ), f32), like(nodal), like(trace), dma((PARTS + 1,))],
        2 * dofs * N * M * EZ, hbm_outs=(0, 1))
    return fields_new.reshape(fields.shape), trace_new.reshape(trace_old.shape)


def solution(mesh):
    placed = (
        P(None, *AXES), P(None, None, *AXES), P(None, None, *AXES), P(None, *AXES), P(*AXES), P(*AXES), P(), P(), P(),
    )
    return jax.shard_map(body, mesh=mesh, in_specs=placed, out_specs=(P(None, *AXES), P(None, None, *AXES)), check_vma=False)
```

```python
import functools

import jax
import jax.numpy as jnp
from jax import lax
from jax.experimental import pallas as pl
from jax.experimental.pallas import tpu as pltpu
from jax.sharding import PartitionSpec as P

AXES = ("gx", "gy", "gz")
TIME_STEP = 0.25
SHIFT_LIMIT = 1e4
PARTS = 4
STRIDE = 8
VMEM_GRANT = 12 * 1024 * 1024
f32, bf16 = jnp.float32, jnp.bfloat16


def pairs(axis, odd):
    size = lax.axis_size(axis)
    route = []
    for i in range(odd, size - 1, 2):
        route += [(i, i + 1), (i + 1, i)]
    return route


def exchange(axes, sends):
    return [[lax.ppermute(v, axis, pairs(axis, odd)) for odd, v in enumerate(s) if pairs(axis, odd)] for axis, s in zip(axes, sends)]


def counts():
    return [sum(bool(pairs(axis, odd)) for odd in (0, 1)) for axis in AXES]


def lane_iota(shape):
    return lax.broadcasted_iota(jnp.int32, shape, len(shape) - 1)


def moved(value, source, target):
    width = value.shape[-1]
    shift = (target - source) % width
    return pltpu.roll(value, shift, value.ndim - 1) if shift else value


def place():
    index = [lax.axis_index(a) for a in AXES]
    parity = [lax.rem(i, 2) for i in index]
    below_top = [(i < lax.axis_size(a) - 1).astype(f32) for i, a in zip(index, AXES)]
    return parity, below_top


def split(value):
    high = value.astype(bf16)
    return high, (value - high.astype(f32)).astype(bf16)


class Geometry:
    def __init__(self, F, EX, EY, EZ):
        self.F, self.EX, self.EY, self.EZ = F, EX, EY, EZ
        self.M = EX * EY


def at_rows(geo, s, m):
    return slice(s * geo.F, (s + 1) * geo.F), slice(m * geo.EZ, (m + 1) * geo.EZ)


def lanes_of(geo):
    lane = lane_iota((geo.F, geo.EZ))
    return lane, lane % STRIDE, lane // (STRIDE * geo.EY), (lane // STRIDE) % geo.EY


def part_of(geo, k, count):
    return slice(k * geo.F, k * geo.F + (geo.F if k < count else 8))


def fold(geo, a, value):
    lane = lane_iota((8, geo.EZ))
    unit = geo.EY * STRIDE if a == 0 else STRIDE
    slot = lane // unit if a == 0 else (lane % (geo.EY * STRIDE)) // unit
    out = jnp.zeros((8, geo.EZ), f32)
    for q in range(geo.F // 8):
        out = jnp.where(slot == q, moved(value[8 * q:8 * q + 8], 0, q * unit), out)
    return out


def unfold(geo, a, value):
    unit = geo.EY * STRIDE if a == 0 else STRIDE
    return jnp.concatenate([moved(value, q * unit, 0) for q in range(geo.F // 8)], 0)


def z_above(geo, z_own, z_pack, m):
    lane = lane_iota((geo.F, geo.EZ))
    return jnp.where(lane == geo.EZ - 1, moved(z_pack, m * STRIDE + 2, geo.EZ - 1), moved(z_own, 1, 0))


def gather_and_apply(geo, own, halo, schur, ghi, glo, wide=None):
    F, EX, EY, EZ, M = geo.F, geo.EX, geo.EY, geo.EZ, geo.M
    hx, hy, hz = halo

    def put(m, blocks):
        for s, block in enumerate(blocks):
            high, low = split(block)
            ghi[at_rows(geo, s, m)] = high
            glo[at_rows(geo, s, m)] = low

    bottom = jnp.zeros((F, EZ), f32)
    lane, column, at_i, at_j = lanes_of(geo)
    for m in range(M):
        i, j = divmod(m, EY)
        z_own = own(2, m)
        put(m, [
            own(0, m), own(0, m + EY) if i + 1 < EX else hx(j),
            own(1, m), own(1, m + 1) if j + 1 < EY else hy(i),
            z_own, z_above(geo, z_own, hz, m),
        ])
        if wide:
            bottom = jnp.where(lane == m * STRIDE + 1, moved(z_own, 0, m * STRIDE + 1), bottom)
    if wide:
        x, y, hx_pack, hy_pack = wide
        put(M, [
            x, jnp.where(at_i == EX - 1, moved(hx_pack, 0, (EX - 1) * EY * STRIDE), moved(x, EY * STRIDE, 0)),
            y, jnp.where(at_j == EY - 1, moved(hy_pack, 0, (EY - 1) * STRIDE), moved(y, STRIDE, 0)),
            hz, jnp.where(column == 1, bottom, moved(hz, 1, 0)),
        ])
    n = 6 * F
    both = jnp.dot(schur[...], ghi[...], preferred_element_type=f32)
    return both[:n] + (both[n:] + jnp.dot(schur[:n], glo[...], preferred_element_type=f32))


def spread(geo, y, weight, own_term, sign, out, sends, parity, weight_pack, own_pack, pack_out):
    F, EX, EY, EZ, M = geo.F, geo.EX, geo.EY, geo.EZ, geo.M
    lane, column, at_i, at_j = lanes_of(geo)
    wrow = [weight[m:m + 1] * sign for m in range(M)] + [weight_pack * sign]

    def block(s, m):
        return y[at_rows(geo, s, m)] * wrow[m]

    low = {}
    below = block(5, M)
    top = jnp.zeros((F, EZ), f32)
    for m in range(M):
        i, j = divmod(m, EY)
        vx = own_term(0, m) + block(0, m)
        if i > 0:
            vx = vx + block(1, m - EY)
        else:
            low[0, j] = vx
        out[0, m] = vx
        vy = own_term(1, m) + block(2, m)
        if j > 0:
            vy = vy + block(3, m - 1)
        else:
            low[1, i] = vy
        out[1, m] = vy
        up = block(5, m)
        out[2, m] = own_term(2, m) + block(4, m) + jnp.where(lane == 0, moved(below, m * STRIDE + 1, 0), moved(up, 0, 1))
        top = jnp.where(lane == m * STRIDE + 2, moved(up, EZ - 1, m * STRIDE + 2), top)
    shared = [
        [(low[0, j], block(1, (EX - 1) * EY + j)) for j in range(EY)],
        [(low[1, i], block(3, i * EY + EY - 1)) for i in range(EX)],
    ]
    pack_out[2][...] = own_pack(2) + block(4, M) + jnp.where(column == 2, top, moved(below, 0, 1))
    if 0 in pack_out:
        up = block(1, M)
        v = own_pack(0) + block(0, M)
        pack_out[0][...] = v + jnp.where(at_i > 0, moved(up, 0, EY * STRIDE), 0.0)
        shared[0].append((fold(geo, 0, v), fold(geo, 0, moved(up, (EX - 1) * EY * STRIDE, 0))))
        up = block(3, M)
        v = own_pack(1) + block(2, M)
        pack_out[1][...] = v + jnp.where(at_j > 0, moved(up, 0, STRIDE), 0.0)
        shared[1].append((fold(geo, 1, v), fold(geo, 1, moved(up, (EY - 1) * STRIDE, 0))))
    for a in (0, 1):
        for odd, ref in enumerate(sends[a]):
            for k, (bottom, high) in enumerate(shared[a]):
                ref[part_of(geo, k, (EY, EX)[a])] = jnp.where(parity[a] == odd, high, bottom)


def chosen(refs, parity, read, flip=False):
    values = [read(r) for r in refs]
    if not values:
        return None
    if len(values) == 1:
        values.append(jnp.zeros_like(values[0]))
    first, second = (values[1], values[0]) if flip else values
    return jnp.where(parity == 0, first, second)


def completed(geo, partial, sent, got, parity, below_top, full, halos):
    F, EX, EY, EZ, M = geo.F, geo.EX, geo.EY, geo.EZ, geo.M
    for f in range(3):
        for m in range(M):
            i, j = divmod(m, EY)
            v = partial[f, m]
            if f == 0 and i == 0 and got[0]:
                v = v + chosen(got[0], parity[0], lambda r: r[part_of(geo, j, EY)], True)
            if f == 1 and j == 0 and got[1]:
                v = v + chosen(got[1], parity[1], lambda r: r[part_of(geo, i, EX)], True)
            full[f, m] = v
    for a, n in ((0, EY), (1, EX)):
        for k in range(n):
            halos[a][k] = both_sides(geo, sent[a], got[a], parity[a], below_top[a], part_of(geo, k, n))


def both_sides(geo, sent, got, parity, below_top, k):
    if not got:
        return jnp.zeros((k.stop - k.start, geo.EZ), f32)
    return (chosen(sent, parity, lambda r: r[k]) + chosen(got, parity, lambda r: r[k])) * below_top


def folded(total, value):
    v = value.reshape(value.shape[0] // 8, 8, value.shape[1]).sum(0)
    return v if total is None else total + v


def rows(ref, geo, f, m):
    return ref[pl.ds(f * geo.F * geo.M + m, geo.F, stride=geo.M), :]


def kernel_pack(geo, trace, load, diag, fine, coeff, pack, vtrace, vload, vdiag, vfine, vcoeff, sems):
    F, EZ, M = geo.F, geo.EZ, geo.M
    for c in fetch([(trace, vtrace), (load, vload), (diag, vdiag), (fine, vfine), (coeff, vcoeff)], sems):
        c.wait()
    half = EZ // 2

    def packed(parts):
        shape = parts[0].shape
        lane = lane_iota(shape)
        out = jnp.zeros(shape, f32)
        for m, part in enumerate(parts):
            start = (m // M) * half + (m % M) * STRIDE
            out = jnp.where((lane >= start) & (lane < start + 5), moved(part, 0, start + 2), out)
        return out

    for f in range(3):
        pack[f * F:(f + 1) * F] = packed([rows(v, geo, f, m) for v in (vtrace, vload) for m in range(M)])
    weight = vfine[...].astype(f32) * vcoeff[...]
    lines = [packed([vdiag[f * M + m:f * M + m + 1] for m in range(M)]) for f in range(3)]
    lines.append(packed([weight[m:m + 1] for m in range(M)]))
    for k in range(8):
        pack[3 * F + k:3 * F + k + 1] = lines[min(k, 3)]


def kernel_wide(geo, n, trace, _, *refs):
    got, (trace_pack, own_pack, lines, sx, sy) = take(refs, n[2:], 5)
    F, EX, EY, EZ = geo.F, geo.EX, geo.EY, geo.EZ
    parity, _ = place()
    lane = lane_iota((F, EZ))

    def mixed(rows_at):
        if not got[0]:
            return jnp.zeros((F, EZ), f32)[:rows_at.stop - rows_at.start]
        below = chosen(got[0], parity[2], lambda r: r[rows_at], True)
        above = chosen(got[0], parity[2], lambda r: r[rows_at])
        return jnp.where(lane[:below.shape[0]] % STRIDE < 2, below, above)

    lines[...] = mixed(slice(3 * F, 3 * F + 8))
    for f in range(3):
        v = mixed(slice(f * F, (f + 1) * F))
        old = jnp.where(lane < EZ // 2, v, 0.0)
        load = jnp.where(lane < EZ // 2, moved(v, EZ // 2, 0), 0.0)
        trace_pack[f] = old
        own_pack[f] = load - lines[f:f + 1] * old
        if f < 2:
            ref, count, step = ((sx, EY, 1), (sy, EX, EY))[f]
            for k in range(count):
                ref[part_of(geo, k, count)] = rows(trace, geo, f, k * step)
            ref[part_of(geo, count, count)] = fold(geo, f, old)


def take(refs, *sizes):
    refs = list(refs)
    out = []
    for s in sizes:
        if isinstance(s, (list, tuple)):
            group = []
            for n in s:
                group.append([refs.pop(0) for _ in range(n)])
            out.append(group)
        else:
            out.append([refs.pop(0) for _ in range(s)])
    assert not refs
    return out


def fetch(pairs, sems):
    copies = [pltpu.make_async_copy(src, dst, sems.at[k]) for k, (src, dst) in enumerate(pairs)]
    for c in copies:
        c.start()
    return copies


def kernel_prepare(geo, trace, load, diag_in, fine, coeff, schur, own, diag, weight, matrix, vload, vfine, vcoeff, vschur, sems):
    copies = fetch([(load, vload), (diag_in, diag), (fine, vfine), (coeff, vcoeff), (schur, vschur)], sems)
    for c in copies:
        c.wait()
    weight[...] = vfine[...].astype(f32) * vcoeff[...]
    n = 6 * geo.F
    matrix[:n], matrix[n:] = split(vschur[...])
    for f in range(3):
        for m in range(geo.M):
            own[f, m] = rows(vload, geo, f, m) - diag[f * geo.M + m:f * geo.M + m + 1] * rows(trace, geo, f, m)


def kernel_start(geo, n, trace, own, weight, schur, _, trace_pack, own_pack, lines, *refs):
    got, halos, (partial, partial_pack), sends, (ghi, glo) = take(refs, n[:2], 2, 2, n[:2], 2)
    F, EX, EY, EZ = geo.F, geo.EX, geo.EY, geo.EZ
    parity, _ = place()

    def above(a, k):
        at = part_of(geo, k, (EY, EX)[a])
        return chosen(got[a], parity[a], lambda r: r[at]) if got[a] else jnp.zeros((at.stop - at.start, EZ), f32)

    for a, count in ((0, EY), (1, EX)):
        for k in range(count):
            halos[a][k] = above(a, k)
    halo = (lambda j: halos[0][j], lambda i: halos[1][i], trace_pack[2])
    wide = (trace_pack[0], trace_pack[1], unfold(geo, 0, above(0, EY)), unfold(geo, 1, above(1, EX)))
    y = gather_and_apply(geo, lambda f, m: rows(trace, geo, f, m), halo, schur, ghi, glo, wide)
    spread(geo, y, weight[...], lambda f, m: own[f, m], -1.0, partial, sends, parity,
           lines[3:4], lambda f: own_pack[f], {f: partial_pack.at[f] for f in range(3)})


def accumulate(total, value):
    return value if total is None else total + value


def kernel_middle(geo, n, partial, partial_pack, diag, weight, schur, lines, *refs):
    sent, got, (full, full_z), halos, (image, image_z), sends, (dots,), (ghi, glo) = take(refs, n[:2], n[:2], 2, 2, 2, n[:2], 1, 2)
    F, EX, EY, EZ, M = geo.F, geo.EX, geo.EY, geo.EZ, geo.M
    parity, below_top = place()
    completed(geo, partial, sent, got, parity, below_top, full, halos)
    lane, column, at_i, at_j = lanes_of(geo)
    packs = []
    for a, edge, count in ((0, at_i == 0, EY), (1, at_j == 0, EX)):
        v = partial_pack[a]
        if got[a]:
            v = v + jnp.where(edge, unfold(geo, a, chosen(got[a], parity[a], lambda r: r[part_of(geo, count, count)], True)), 0.0)
        packs.append(v)
    beside = [unfold(geo, a, both_sides(geo, sent[a], got[a], parity[a], below_top[a], part_of(geo, k, k))) for a, k in ((0, EY), (1, EX))]
    wide = (*packs, *beside)
    full_z[...] = jnp.where(column < 2, partial_pack[2], partial_pack[2] * below_top[2])
    halo = (lambda j: halos[0][j], lambda i: halos[1][i], full_z[...])
    y = gather_and_apply(geo, lambda f, m: full[f, m], halo, schur, ghi, glo, wide)
    squares = energy = None
    for f in range(3):
        for m in range(M):
            vv = folded(None, full[f, m] * full[f, m])
            squares = accumulate(squares, vv)
            energy = accumulate(energy, vv * diag[f * M + m:f * M + m + 1])
    for m in range(M):
        part = None
        for s in range(6):
            at = at_rows(geo, s, m)
            part = folded(part, (ghi[at].astype(f32) + glo[at].astype(f32)) * y[at])
        energy = energy + part * weight[m:m + 1]
    dots[0], dots[1] = squares, energy
    spread(geo, y, weight[...], lambda f, m: diag[f * M + m:f * M + m + 1] * full[f, m], 1.0, image, sends, parity,
           lines[3:4], lambda f: lines[f:f + 1] * full_z[...], {2: image_z})
    image_z[...] = image_z[...] * below_top[2]


def kernel_last(geo, n, partial, image_z, diag, weight, schur, dots, r, hxr, hyr, hzr, *refs):
    sent, got, (full,), halos, (message,), (ghi, glo) = take(refs, n[:2], n[:2], 1, 2, 1, 2)
    F, EX, EY, EZ, M = geo.F, geo.EX, geo.EY, geo.EZ, geo.M
    parity, below_top = place()
    completed(geo, partial, sent, got, parity, below_top, full, halos)
    along = None
    for f in range(3):
        for m in range(M):
            along = folded(along, r[f, m] * full[f, m])
    squares = jnp.sum(dots[0], keepdims=True)
    along = jnp.sum(along, keepdims=True)
    shift = jnp.where(squares > 0, jnp.clip(along / squares, -SHIFT_LIMIT, SHIFT_LIMIT), 0.0)
    halo = (lambda j: halos[0][j] - shift * hxr[j], lambda i: halos[1][i] - shift * hyr[i], image_z[...] - shift * hzr[...])
    y = gather_and_apply(geo, lambda f, m: full[f, m] - shift * r[f, m], halo, schur, ghi, glo)
    rp = pp = erp = epp = None
    for f in range(3):
        for m in range(M):
            v = r[f, m]
            p = full[f, m] - shift * v
            d = diag[f * M + m:f * M + m + 1]
            a, b = folded(None, v * p), folded(None, p * p)
            rp, pp = accumulate(rp, a), accumulate(pp, b)
            erp, epp = accumulate(erp, a * d), accumulate(epp, b * d)
    for m in range(M):
        i, j = divmod(m, EY)
        blocks = [
            r[0, m], r[0, m + EY] if i + 1 < EX else hxr[j],
            r[1, m], r[1, m + 1] if j + 1 < EY else hyr[i],
            r[2, m], z_above(geo, r[2, m], hzr[...], m),
        ]
        one = two = None
        for s, block in enumerate(blocks):
            at = at_rows(geo, s, m)
            one = folded(one, block * y[at])
            two = folded(two, (ghi[at].astype(f32) + glo[at].astype(f32)) * y[at])
        erp = erp + one * weight[m:m + 1]
        epp = epp + two * weight[m:m + 1]
    lane = lane_iota((1, EZ))
    line = jnp.where(lane == 0, shift, jnp.where(lane == 1, squares, 0.0))
    for k, v in enumerate((rp, pp, dots[1], erp, epp)):
        line = jnp.where(lane == k + 2, jnp.sum(v, keepdims=True), line)
    message[...] = jnp.broadcast_to(line, message.shape)


def step_sizes(rows_of_devices):
    lanes = lane_iota(rows_of_devices.shape)
    theta, rr, rp, pp, err, erp, epp = [jnp.sum(jnp.where(lanes == k, rows_of_devices, 0.0), 1, keepdims=True) for k in range(7)]

    def total(v):
        return jnp.sum(v, 0, keepdims=True)

    old = total(rr)
    alpha = old / total(err)
    u = 1.0 - alpha * theta
    new = total(u * u * rr - 2.0 * u * alpha * rp + alpha * alpha * pp)
    beta = new / old
    c = u + beta
    energy = total(c * c * err - 2.0 * c * alpha * erp + alpha * alpha * epp)
    second = jnp.where(energy > 0, new / energy, 0.0)
    return alpha + second * (1.0 + beta), -alpha * second


def kernel_volume(geo, fields, fine, operator, lift_in, base, lift, plain, vfields, vfine, voperator, vlift, sems):
    M, EZ = geo.M, geo.EZ
    dofs = operator.shape[0]
    for c in fetch([(fields, vfields), (fine, vfine), (operator, voperator), (lift_in, vlift)], sems):
        c.wait()
    plain[...] = vfields[...].astype(f32)
    lift[...] = vlift[...].T
    nodal = [plain[pl.ds(m, dofs, stride=M), :] for m in range(M)]
    volume = jnp.dot(voperator[...], jnp.concatenate([v.astype(bf16) for v in nodal], 1), preferred_element_type=f32)
    coarse = 1.0 - vfine[...].astype(f32)
    for m in range(M):
        base[m] = nodal[m] + (TIME_STEP * coarse[m:m + 1]) * volume[:, m * EZ:(m + 1) * EZ]


def kernel_finish(geo, message, trace, base, fine, lift, r, q, *refs):
    (hx, hy, hz), (hxr, hyr, hzr), (hxq, hyq, hzq), (fields_out, trace_out), (g, plain, fields_new, trace_new, sems) = take(refs, 3, 3, 3, 2, 5)
    F, EX, EY, EZ, M = geo.F, geo.EX, geo.EY, geo.EZ, geo.M
    cr, cq = step_sizes(message[...])
    flag = fine[...].astype(f32)
    z_step = cr * hzr[...] + cq * hzq[...]
    for m in range(M):
        i, j = divmod(m, EY)
        mark = flag[m:m + 1]

        def old_step(f, k):
            return rows(trace, geo, f, k), cr * r[f, k] + cq * q[f, k]

        ox, sx = old_step(0, m)
        oy, sy = old_step(1, m)
        oz, sz = old_step(2, m)
        for f, (o, s) in enumerate(((ox, sx), (oy, sy), (oz, sz))):
            trace_new[pl.ds(f * F * M + m, F, stride=M), :] = o + s
        up_x = old_step(0, m + EY) if i + 1 < EX else (hx[j], cr * hxr[j] + cq * hxq[j])
        up_y = old_step(1, m + 1) if j + 1 < EY else (hy[i], cr * hyr[i] + cq * hyq[i])
        up_z = (z_above(geo, oz, hz[2], m), z_above(geo, sz, z_step, m))
        for s, (o, step) in enumerate(((ox, sx), up_x, (oy, sy), up_y, (oz, sz), up_z)):
            g[s * F:(s + 1) * F, m * EZ:(m + 1) * EZ] = (o + mark * step).astype(bf16)
    copies = [pltpu.make_async_copy(trace_new, trace_out, sems.at[0])]
    copies[0].start()
    dofs = lift.shape[0]
    part = dofs // PARTS
    for k in range(PARTS):
        lifted = jnp.dot(lift[k * part:(k + 1) * part], g[...], preferred_element_type=f32)
        for m in range(M):
            plain[pl.ds(k * part * M + m, part, stride=M), :] = base[m, k * part:(k + 1) * part] + TIME_STEP * lifted[:, m * EZ:(m + 1) * EZ]
        some = pl.ds(k * part * M, part * M)
        fields_new[some] = plain[some].astype(bf16)
        copies.append(pltpu.make_async_copy(fields_new.at[some], fields_out.at[some], sems.at[k + 1]))
        copies[-1].start()
    for c in copies:
        c.wait()


VMEM, HBM = pltpu.MemorySpace.VMEM, pltpu.MemorySpace.HBM


def call(kernel, outs, args, scratch, flops, hbm_args=(), hbm_outs=()):
    def specs(count, in_hbm):
        return [pl.BlockSpec(memory_space=HBM if k in in_hbm else VMEM) for k in range(count)]

    args = [pltpu.with_memory_space_constraint(v, HBM) if k in hbm_args else v for k, v in enumerate(args)]
    return pl.pallas_call(
        kernel,
        out_shape=[(HBM if k in hbm_outs else jax.ShapeDtypeStruct)(s, d) for k, (s, d) in enumerate(outs)],
        in_specs=specs(len(args), hbm_args),
        out_specs=specs(len(outs), hbm_outs),
        scratch_shapes=scratch,
        cost_estimate=pl.CostEstimate(flops=flops, bytes_accessed=1 << 20, transcendentals=0),
        compiler_params=pltpu.CompilerParams(vmem_limit_bytes=VMEM_GRANT),
    )(*args)


def flat(groups):
    return [v for group in groups for v in group if v is not None]


def like(array):
    return pltpu.VMEM(array.shape, array.dtype)


def body(fields, trace_old, face_load, face_diag, fine_flag, coeff, volume_op, lift_op, schur_op):
    _, F, EX, EY, EZ = trace_old.shape
    geo = Geometry(F, EX, EY, EZ)
    M, dofs, N = geo.M, fields.shape[0], 6 * F
    devices = 1
    for a in AXES:
        devices *= lax.axis_size(a)
    n = counts()
    trace = trace_old.reshape(3 * F * M, EZ)
    load = face_load.reshape(3 * F * M, EZ)
    diag_in = face_diag.reshape(3 * M, EZ)
    fine = fine_flag.reshape(M, EZ)
    scale = coeff.reshape(M, EZ)
    nodal = fields.reshape(dofs * M, EZ)
    slab = [(EY, F, EZ), (EX, F, EZ)]
    slab_sent = [(EY * F, EZ), (EX * F, EZ)]
    slab_wide = [(EY * F + 8, EZ), (EX * F + 8, EZ)]
    full, pack, line = (3, M, F, EZ), (3, F, EZ), (8, EZ)
    halo_outs = [(s, f32) for s in slab]
    flops = 2 * 3 * N * N * M * EZ
    dma = pltpu.SemaphoreType.DMA

    def halves(blocks):
        return [pltpu.VMEM((N, blocks * EZ), bf16)] * 2

    def send_outs(shapes):
        return [(s, f32) for s, k in zip(shapes, n) for _ in range(k)]

    def grouped(values):
        values = list(values)
        return [[values.pop(0) for _ in range(k)] for k in n[:2]]

    packed, held = call(functools.partial(kernel_pack, geo), [((3 * F + 8, EZ), f32), (trace.shape, f32)], [trace, load, diag_in, fine, scale],
                        [like(load), like(diag_in), like(fine), like(scale), dma((5,))], 1 << 20, hbm_args=range(5))
    got = exchange(AXES[2:], [[packed, packed]])
    own, diag, weight, schur = call(
        functools.partial(kernel_prepare, geo), [(full, f32), ((3 * M, EZ), f32), ((M, EZ), f32), ((2 * N, N), bf16)],
        [held, load, diag_in, fine, scale, schur_op], [like(load), like(fine), like(scale), like(schur_op), dma((5,))],
        flops, hbm_args=(1, 2, 3, 4, 5))
    base, lift = call(
        functools.partial(kernel_volume, geo), [((M, dofs, EZ), f32), (lift_op.shape, bf16)], [nodal, fine, volume_op, lift_op.T],
        [pltpu.VMEM((dofs * M, EZ), f32), like(nodal), like(fine), like(volume_op), like(lift_op.T), dma((4,))],
        2 * dofs * dofs * M * EZ, hbm_args=(0, 1, 2, 3))
    trace_pack, own_pack, lines, sx, sy = call(
        functools.partial(kernel_wide, geo, n), [(pack, f32), (pack, f32), (line, f32)] + [(s, f32) for s in slab_wide],
        [held, weight] + flat(got), [], 1 << 20)
    got = exchange(AXES[:2], [[sx, sx], [sy, sy]])
    out = call(functools.partial(kernel_start, geo, n), halo_outs + [(full, f32), (pack, f32)] + send_outs(slab_wide),
               [held, own, weight, schur, base, trace_pack, own_pack, lines] + flat(got), halves(M + 1), flops)
    halo_old, partial, partial_pack, sent = [*out[:2], trace_pack], out[2], out[3], grouped(out[4:])
    got = exchange(AXES[:2], sent)
    out = call(functools.partial(kernel_middle, geo, n),
               [(full, f32), ((F, EZ), f32)] + halo_outs + [(full, f32), ((F, EZ), f32)] + send_outs(slab_sent) + [((2, 8, EZ), f32)],
               [partial, partial_pack, diag, weight, schur, lines] + flat(sent) + flat(got), halves(M + 1), flops)
    r, r_z, partial, image_z, sent, dots = out[0], out[1], out[4], out[5], grouped(out[6:-1]), out[-1]
    halo_r = [*out[2:4], r_z]
    got = exchange(AXES[:2], sent)
    out = call(functools.partial(kernel_last, geo, n), [(full, f32)] + halo_outs + [((devices, EZ), f32)],
               [partial, image_z, diag, weight, schur, dots, r, *halo_r] + flat(sent) + flat(got), halves(M), flops)
    q, halo_q, message = out[0], [*out[1:3], image_z], out[3]
    message = lax.all_to_all(message, AXES, 0, 0, tiled=True)
    fields_new, trace_new = call(
        functools.partial(kernel_finish, geo), [((dofs * M, EZ), bf16), ((3 * F * M, EZ), f32)],
        [message, trace, base, fine, lift, r, q, *halo_old, *halo_r, *halo_q],
        [pltpu.VMEM((N, M * EZ), bf16), pltpu.VMEM((dofs * M, EZ), f32), like(nodal), like(trace), dma((PARTS + 1,))],
        2 * dofs * N * M * EZ, hbm_outs=(0, 1))
    return fields_new.reshape(fields.shape), trace_new.reshape(trace_old.shape)


def solution(mesh):
    placed = (
        P(None, *AXES), P(None, None, *AXES), P(None, None, *AXES), P(None, *AXES), P(*AXES), P(*AXES), P(), P(), P(),
    )
    return jax.shard_map(body, mesh=mesh, in_specs=placed, out_specs=(P(None, *AXES), P(None, None, *AXES)), check_vma=False)
```

```python
import functools

import jax
import jax.numpy as jnp
from jax import lax
from jax.experimental import pallas as pl
from jax.experimental.pallas import tpu as pltpu
from jax.sharding import PartitionSpec as P

AXES = ("gx", "gy", "gz")
TIME_STEP = 0.25
SHIFT_LIMIT = 1e4
PARTS = 4
STRIDE = 8
VMEM_GRANT = 12 * 1024 * 1024
f32, bf16 = jnp.float32, jnp.bfloat16


def pairs(axis, odd):
    size = lax.axis_size(axis)
    route = []
    for i in range(odd, size - 1, 2):
        route += [(i, i + 1), (i + 1, i)]
    return route


def exchange(axes, sends):
    return [[lax.ppermute(v, axis, pairs(axis, odd)) for odd, v in enumerate(s) if pairs(axis, odd)] for axis, s in zip(axes, sends)]


def counts():
    return [sum(bool(pairs(axis, odd)) for odd in (0, 1)) for axis in AXES]


def lane_iota(shape):
    return lax.broadcasted_iota(jnp.int32, shape, len(shape) - 1)


def moved(value, source, target):
    width = value.shape[-1]
    shift = (target - source) % width
    return pltpu.roll(value, shift, value.ndim - 1) if shift else value


def place():
    index = [lax.axis_index(a) for a in AXES]
    parity = [lax.rem(i, 2) for i in index]
    below_top = [(i < lax.axis_size(a) - 1).astype(f32) for i, a in zip(index, AXES)]
    return parity, below_top


def split(value):
    high = value.astype(bf16)
    return high, (value - high.astype(f32)).astype(bf16)


class Geometry:
    def __init__(self, F, EX, EY, EZ):
        self.F, self.EX, self.EY, self.EZ = F, EX, EY, EZ
        self.M = EX * EY


def at_rows(geo, s, m):
    return slice(s * geo.F, (s + 1) * geo.F), slice(m * geo.EZ, (m + 1) * geo.EZ)


def lanes_of(geo):
    lane = lane_iota((geo.F, geo.EZ))
    return lane, lane % STRIDE, lane // (STRIDE * geo.EY), (lane // STRIDE) % geo.EY


def part_of(geo, k, count):
    return slice(k * geo.F, k * geo.F + (geo.F if k < count else 8))


def fold(geo, a, value):
    lane = lane_iota((8, geo.EZ))
    unit = geo.EY * STRIDE if a == 0 else STRIDE
    slot = lane // unit if a == 0 else (lane % (geo.EY * STRIDE)) // unit
    out = jnp.zeros((8, geo.EZ), f32)
    for q in range(geo.F // 8):
        out = jnp.where(slot == q, moved(value[8 * q:8 * q + 8], 0, q * unit), out)
    return out


def unfold(geo, a, value):
    unit = geo.EY * STRIDE if a == 0 else STRIDE
    return jnp.concatenate([moved(value, q * unit, 0) for q in range(geo.F // 8)], 0)


def z_above(geo, z_own, z_pack, m):
    lane = lane_iota((geo.F, geo.EZ))
    return jnp.where(lane == geo.EZ - 1, moved(z_pack, m * STRIDE + 2, geo.EZ - 1), moved(z_own, 1, 0))


def gather_and_apply(geo, own, halo, schur, ghi, glo, wide=None):
    F, EX, EY, EZ, M = geo.F, geo.EX, geo.EY, geo.EZ, geo.M
    hx, hy, hz = halo

    def put(m, blocks):
        for s, block in enumerate(blocks):
            high, low = split(block)
            ghi[at_rows(geo, s, m)] = high
            glo[at_rows(geo, s, m)] = low

    bottom = jnp.zeros((F, EZ), f32)
    lane, column, at_i, at_j = lanes_of(geo)
    for m in range(M):
        i, j = divmod(m, EY)
        z_own = own(2, m)
        put(m, [
            own(0, m), own(0, m + EY) if i + 1 < EX else hx(j),
            own(1, m), own(1, m + 1) if j + 1 < EY else hy(i),
            z_own, z_above(geo, z_own, hz, m),
        ])
        if wide:
            bottom = jnp.where(lane == m * STRIDE + 1, moved(z_own, 0, m * STRIDE + 1), bottom)
    if wide:
        x, y, hx_pack, hy_pack = wide
        put(M, [
            x, jnp.where(at_i == EX - 1, moved(hx_pack, 0, (EX - 1) * EY * STRIDE), moved(x, EY * STRIDE, 0)),
            y, jnp.where(at_j == EY - 1, moved(hy_pack, 0, (EY - 1) * STRIDE), moved(y, STRIDE, 0)),
            hz, jnp.where(column == 1, bottom, moved(hz, 1, 0)),
        ])
    n = 6 * F
    both = jnp.dot(schur[...], ghi[...], preferred_element_type=f32)
    return both[:n] + (both[n:] + jnp.dot(schur[:n], glo[...], preferred_element_type=f32))


def spread(geo, y, weight, own_term, sign, out, sends, parity, weight_pack, own_pack, pack_out):
    F, EX, EY, EZ, M = geo.F, geo.EX, geo.EY, geo.EZ, geo.M
    lane, column, at_i, at_j = lanes_of(geo)
    wrow = [weight[m:m + 1] * sign for m in range(M)] + [weight_pack * sign]

    def block(s, m):
        return y[at_rows(geo, s, m)] * wrow[m]

    low = {}
    below = block(5, M)
    top = jnp.zeros((F, EZ), f32)
    for m in range(M):
        i, j = divmod(m, EY)
        vx = own_term(0, m) + block(0, m)
        if i > 0:
            vx = vx + block(1, m - EY)
        else:
            low[0, j] = vx
        out[0, m] = vx
        vy = own_term(1, m) + block(2, m)
        if j > 0:
            vy = vy + block(3, m - 1)
        else:
            low[1, i] = vy
        out[1, m] = vy
        up = block(5, m)
        out[2, m] = own_term(2, m) + block(4, m) + jnp.where(lane == 0, moved(below, m * STRIDE + 1, 0), moved(up, 0, 1))
        top = jnp.where(lane == m * STRIDE + 2, moved(up, EZ - 1, m * STRIDE + 2), top)
    shared = [
        [(low[0, j], block(1, (EX - 1) * EY + j)) for j in range(EY)],
        [(low[1, i], block(3, i * EY + EY - 1)) for i in range(EX)],
    ]
    pack_out[2][...] = own_pack(2) + block(4, M) + jnp.where(column == 2, top, moved(below, 0, 1))
    if 0 in pack_out:
        up = block(1, M)
        v = own_pack(0) + block(0, M)
        pack_out[0][...] = v + jnp.where(at_i > 0, moved(up, 0, EY * STRIDE), 0.0)
        shared[0].append((fold(geo, 0, v), fold(geo, 0, moved(up, (EX - 1) * EY * STRIDE, 0))))
        up = block(3, M)
        v = own_pack(1) + block(2, M)
        pack_out[1][...] = v + jnp.where(at_j > 0, moved(up, 0, STRIDE), 0.0)
        shared[1].append((fold(geo, 1, v), fold(geo, 1, moved(up, (EY - 1) * STRIDE, 0))))
    for a in (0, 1):
        for odd, ref in enumerate(sends[a]):
            for k, (bottom, high) in enumerate(shared[a]):
                ref[part_of(geo, k, (EY, EX)[a])] = jnp.where(parity[a] == odd, high, bottom)


def chosen(refs, parity, read, flip=False):
    values = [read(r) for r in refs]
    if not values:
        return None
    if len(values) == 1:
        values.append(jnp.zeros_like(values[0]))
    first, second = (values[1], values[0]) if flip else values
    return jnp.where(parity == 0, first, second)


def completed(geo, partial, sent, got, parity, below_top, full, halos):
    F, EX, EY, EZ, M = geo.F, geo.EX, geo.EY, geo.EZ, geo.M
    for f in range(3):
        for m in range(M):
            i, j = divmod(m, EY)
            v = partial[f, m]
            if f == 0 and i == 0 and got[0]:
                v = v + chosen(got[0], parity[0], lambda r: r[part_of(geo, j, EY)], True)
            if f == 1 and j == 0 and got[1]:
                v = v + chosen(got[1], parity[1], lambda r: r[part_of(geo, i, EX)], True)
            full[f, m] = v
    for a, n in ((0, EY), (1, EX)):
        for k in range(n):
            halos[a][k] = both_sides(geo, sent[a], got[a], parity[a], below_top[a], part_of(geo, k, n))


def both_sides(geo, sent, got, parity, below_top, k):
    if not got:
        return jnp.zeros((k.stop - k.start, geo.EZ), f32)
    return (chosen(sent, parity, lambda r: r[k]) + chosen(got, parity, lambda r: r[k])) * below_top


def folded(total, value):
    v = value.reshape(value.shape[0] // 8, 8, value.shape[1]).sum(0)
    return v if total is None else total + v


def rows(ref, geo, f, m):
    return ref[pl.ds(f * geo.F * geo.M + m, geo.F, stride=geo.M), :]


def kernel_slabs(geo, trace, held, sx, sy, sems):
    for c in fetch([(trace, held)], sems):
        c.wait()
    for f, (ref, count, step) in enumerate(((sx, geo.EY, 1), (sy, geo.EX, geo.EY))):
        for k in range(count):
            ref[part_of(geo, k, count)] = rows(held, geo, f, k * step)


def packed(geo, parts, start=0, out=None, spread=1):
    slot = lane_iota(parts[0].shape) // STRIDE
    out = jnp.zeros(parts[0].shape, f32) if out is None else out
    for k, part in enumerate(parts):
        at = start + k * spread * STRIDE
        out = jnp.where(slot == at // STRIDE, moved(part, 0, at + 2), out)
    return out


def kernel_pack(geo, n, columns, *refs):
    got, (out,) = take(refs, n[:2], 1)
    parity, _ = place()
    rows_in = columns.shape[0]
    out[:rows_in] = columns[...]
    block = jnp.zeros((geo.F, geo.EZ), f32)
    for a, count, spread in ((0, geo.EY, 1), (1, geo.EX, geo.EY)):
        if got[a]:
            parts = [chosen(got[a], parity[a], lambda r: r[part_of(geo, k, count)]) for k in range(count)]
            block = packed(geo, parts, a * geo.EZ // 2, block, spread)
    out[rows_in:] = block


def take(refs, *sizes):
    refs = list(refs)
    out = []
    for s in sizes:
        if isinstance(s, (list, tuple)):
            group = []
            for n in s:
                group.append([refs.pop(0) for _ in range(n)])
            out.append(group)
        else:
            out.append([refs.pop(0) for _ in range(s)])
    assert not refs
    return out


def fetch(pairs, sems):
    copies = [pltpu.make_async_copy(src, dst, sems.at[k]) for k, (src, dst) in enumerate(pairs)]
    for c in copies:
        c.start()
    return copies


def kernel_prepare(geo, trace, load, diag_in, fine, coeff, schur, own, diag, weight, matrix, columns, vload, vfine, vcoeff, vschur, sems):
    F, M = geo.F, geo.M
    copies = fetch([(load, vload), (diag_in, diag), (fine, vfine), (coeff, vcoeff), (schur, vschur)], sems)
    for c in copies:
        c.wait()
    scale = vfine[...].astype(f32) * vcoeff[...]
    weight[...] = scale
    n = 6 * F
    matrix[:n], matrix[n:] = split(vschur[...])
    for f in range(3):
        for m in range(M):
            own[f, m] = rows(vload, geo, f, m) - diag[f * M + m:f * M + m + 1] * rows(trace, geo, f, m)
        old = packed(geo, [rows(trace, geo, f, m) for m in range(M)])
        columns[f * F:(f + 1) * F] = packed(geo, [own[f, m] for m in range(M)], geo.EZ // 2, old)
    lines = [packed(geo, [diag[f * M + m:f * M + m + 1] for m in range(M)]) for f in range(3)]
    lines.append(packed(geo, [scale[m:m + 1] for m in range(M)]))
    for k in range(8):
        columns[3 * F + k:3 * F + k + 1] = lines[min(k, 3)]


def kernel_start(geo, n, trace, own, weight, schur, _, *refs):
    got, halos, (trace_pack, lines, partial, partial_pack), sends, (ghi, glo) = take(refs, n, 2, 4, n[:2], 2)
    F, EX, EY, EZ = geo.F, geo.EX, geo.EY, geo.EZ
    parity, _ = place()
    lane = lane_iota((F, EZ))

    def mixed(rows_at):
        if not got[2]:
            return jnp.zeros((rows_at.stop - rows_at.start, EZ), f32)
        below = chosen(got[2], parity[2], lambda r: r[rows_at], True)
        above = chosen(got[2], parity[2], lambda r: r[rows_at])
        return jnp.where(lane[:below.shape[0]] % STRIDE < 2, below, above)

    lines[...] = mixed(slice(3 * F, 3 * F + 8))
    own_pack = []
    for f in range(3):
        v = mixed(slice(f * F, (f + 1) * F))
        trace_pack[f] = jnp.where(lane < EZ // 2, v, 0.0)
        own_pack.append(jnp.where(lane < EZ // 2, moved(v, EZ // 2, 0), 0.0))
    beside = mixed(slice(3 * F + 8, 4 * F + 8))
    for a, count in ((0, EY), (1, EX)):
        for k in range(count):
            halos[a][k] = chosen(got[a], parity[a], lambda r: r[part_of(geo, k, count)]) if got[a] else jnp.zeros((F, EZ), f32)
    halo = (lambda j: halos[0][j], lambda i: halos[1][i], trace_pack[2])
    wide = (trace_pack[0], trace_pack[1], beside, moved(beside, EZ // 2, 0))
    y = gather_and_apply(geo, lambda f, m: rows(trace, geo, f, m), halo, schur, ghi, glo, wide)
    spread(geo, y, weight[...], lambda f, m: own[f, m], -1.0, partial, sends, parity,
           lines[3:4], lambda f: own_pack[f], {f: partial_pack.at[f] for f in range(3)})


def accumulate(total, value):
    return value if total is None else total + value


def kernel_middle(geo, n, partial, partial_pack, diag, weight, schur, lines, *refs):
    sent, got, (full, full_z), halos, (image, image_z), sends, (dots,), (ghi, glo) = take(refs, n[:2], n[:2], 2, 2, 2, n[:2], 1, 2)
    F, EX, EY, EZ, M = geo.F, geo.EX, geo.EY, geo.EZ, geo.M
    parity, below_top = place()
    completed(geo, partial, sent, got, parity, below_top, full, halos)
    lane, column, at_i, at_j = lanes_of(geo)
    packs = []
    for a, edge, count in ((0, at_i == 0, EY), (1, at_j == 0, EX)):
        v = partial_pack[a]
        if got[a]:
            v = v + jnp.where(edge, unfold(geo, a, chosen(got[a], parity[a], lambda r: r[part_of(geo, count, count)], True)), 0.0)
        packs.append(v)
    beside = [unfold(geo, a, both_sides(geo, sent[a], got[a], parity[a], below_top[a], part_of(geo, k, k))) for a, k in ((0, EY), (1, EX))]
    wide = (*packs, *beside)
    full_z[...] = jnp.where(column < 2, partial_pack[2], partial_pack[2] * below_top[2])
    halo = (lambda j: halos[0][j], lambda i: halos[1][i], full_z[...])
    y = gather_and_apply(geo, lambda f, m: full[f, m], halo, schur, ghi, glo, wide)
    squares = energy = None
    for f in range(3):
        for m in range(M):
            vv = folded(None, full[f, m] * full[f, m])
            squares = accumulate(squares, vv)
            energy = accumulate(energy, vv * diag[f * M + m:f * M + m + 1])
    for m in range(M):
        part = None
        for s in range(6):
            at = at_rows(geo, s, m)
            part = folded(part, (ghi[at].astype(f32) + glo[at].astype(f32)) * y[at])
        energy = energy + part * weight[m:m + 1]
    dots[0], dots[1] = squares, energy
    spread(geo, y, weight[...], lambda f, m: diag[f * M + m:f * M + m + 1] * full[f, m], 1.0, image, sends, parity,
           lines[3:4], lambda f: lines[f:f + 1] * full_z[...], {2: image_z})
    image_z[...] = image_z[...] * below_top[2]


def kernel_last(geo, n, partial, image_z, diag, weight, schur, dots, r, hxr, hyr, hzr, *refs):
    sent, got, (full,), halos, (message,), (ghi, glo) = take(refs, n[:2], n[:2], 1, 2, 1, 2)
    F, EX, EY, EZ, M = geo.F, geo.EX, geo.EY, geo.EZ, geo.M
    parity, below_top = place()
    completed(geo, partial, sent, got, parity, below_top, full, halos)
    along = None
    for f in range(3):
        for m in range(M):
            along = folded(along, r[f, m] * full[f, m])
    squares = jnp.sum(dots[0], keepdims=True)
    along = jnp.sum(along, keepdims=True)
    shift = jnp.where(squares > 0, jnp.clip(along / squares, -SHIFT_LIMIT, SHIFT_LIMIT), 0.0)
    halo = (lambda j: halos[0][j] - shift * hxr[j], lambda i: halos[1][i] - shift * hyr[i], image_z[...] - shift * hzr[...])
    y = gather_and_apply(geo, lambda f, m: full[f, m] - shift * r[f, m], halo, schur, ghi, glo)
    rp = pp = erp = epp = None
    for f in range(3):
        for m in range(M):
            v = r[f, m]
            p = full[f, m] - shift * v
            d = diag[f * M + m:f * M + m + 1]
            a, b = folded(None, v * p), folded(None, p * p)
            rp, pp = accumulate(rp, a), accumulate(pp, b)
            erp, epp = accumulate(erp, a * d), accumulate(epp, b * d)
    for m in range(M):
        i, j = divmod(m, EY)
        blocks = [
            r[0, m], r[0, m + EY] if i + 1 < EX else hxr[j],
            r[1, m], r[1, m + 1] if j + 1 < EY else hyr[i],
            r[2, m], z_above(geo, r[2, m], hzr[...], m),
        ]
        one = two = None
        for s, block in enumerate(blocks):
            at = at_rows(geo, s, m)
            one = folded(one, block * y[at])
            two = folded(two, (ghi[at].astype(f32) + glo[at].astype(f32)) * y[at])
        erp = erp + one * weight[m:m + 1]
        epp = epp + two * weight[m:m + 1]
    lane = lane_iota((1, EZ))
    line = jnp.where(lane == 0, shift, jnp.where(lane == 1, squares, 0.0))
    for k, v in enumerate((rp, pp, dots[1], erp, epp)):
        line = jnp.where(lane == k + 2, jnp.sum(v, keepdims=True), line)
    message[...] = jnp.broadcast_to(line, message.shape)


def step_sizes(rows_of_devices):
    lanes = lane_iota(rows_of_devices.shape)
    theta, rr, rp, pp, err, erp, epp = [jnp.sum(jnp.where(lanes == k, rows_of_devices, 0.0), 1, keepdims=True) for k in range(7)]

    def total(v):
        return jnp.sum(v, 0, keepdims=True)

    old = total(rr)
    alpha = old / total(err)
    u = 1.0 - alpha * theta
    new = total(u * u * rr - 2.0 * u * alpha * rp + alpha * alpha * pp)
    beta = new / old
    c = u + beta
    energy = total(c * c * err - 2.0 * c * alpha * erp + alpha * alpha * epp)
    second = jnp.where(energy > 0, new / energy, 0.0)
    return alpha + second * (1.0 + beta), -alpha * second


def kernel_volume(geo, fields, fine, operator, lift_in, base, lift, plain, vfields, vfine, voperator, vlift, sems):
    M, EZ = geo.M, geo.EZ
    dofs = operator.shape[0]
    for c in fetch([(fields, vfields), (fine, vfine), (operator, voperator), (lift_in, vlift)], sems):
        c.wait()
    plain[...] = vfields[...].astype(f32)
    lift[...] = vlift[...].T
    nodal = [plain[pl.ds(m, dofs, stride=M), :] for m in range(M)]
    volume = jnp.dot(voperator[...], jnp.concatenate([v.astype(bf16) for v in nodal], 1), preferred_element_type=f32)
    coarse = 1.0 - vfine[...].astype(f32)
    for m in range(M):
        base[m] = nodal[m] + (TIME_STEP * coarse[m:m + 1]) * volume[:, m * EZ:(m + 1) * EZ]


def kernel_finish(geo, message, trace, base, fine, lift, r, q, *refs):
    (hx, hy, hz), (hxr, hyr, hzr), (hxq, hyq, hzq), (fields_out, trace_out), (g, plain, fields_new, trace_new, sems) = take(refs, 3, 3, 3, 2, 5)
    F, EX, EY, EZ, M = geo.F, geo.EX, geo.EY, geo.EZ, geo.M
    cr, cq = step_sizes(message[...])
    flag = fine[...].astype(f32)
    z_step = cr * hzr[...] + cq * hzq[...]
    for m in range(M):
        i, j = divmod(m, EY)
        mark = flag[m:m + 1]

        def old_step(f, k):
            return rows(trace, geo, f, k), cr * r[f, k] + cq * q[f, k]

        ox, sx = old_step(0, m)
        oy, sy = old_step(1, m)
        oz, sz = old_step(2, m)
        for f, (o, s) in enumerate(((ox, sx), (oy, sy), (oz, sz))):
            trace_new[pl.ds(f * F * M + m, F, stride=M), :] = o + s
        up_x = old_step(0, m + EY) if i + 1 < EX else (hx[j], cr * hxr[j] + cq * hxq[j])
        up_y = old_step(1, m + 1) if j + 1 < EY else (hy[i], cr * hyr[i] + cq * hyq[i])
        up_z = (z_above(geo, oz, hz[2], m), z_above(geo, sz, z_step, m))
        for s, (o, step) in enumerate(((ox, sx), up_x, (oy, sy), up_y, (oz, sz), up_z)):
            g[s * F:(s + 1) * F, m * EZ:(m + 1) * EZ] = (o + mark * step).astype(bf16)
    copies = [pltpu.make_async_copy(trace_new, trace_out, sems.at[0])]
    copies[0].start()
    dofs = lift.shape[0]
    part = dofs // PARTS
    for k in range(PARTS):
        lifted = jnp.dot(lift[k * part:(k + 1) * part], g[...], preferred_element_type=f32)
        for m in range(M):
            plain[pl.ds(k * part * M + m, part, stride=M), :] = base[m, k * part:(k + 1) * part] + TIME_STEP * lifted[:, m * EZ:(m + 1) * EZ]
        some = pl.ds(k * part * M, part * M)
        fields_new[some] = plain[some].astype(bf16)
        copies.append(pltpu.make_async_copy(fields_new.at[some], fields_out.at[some], sems.at[k + 1]))
        copies[-1].start()
    for c in copies:
        c.wait()


VMEM, HBM = pltpu.MemorySpace.VMEM, pltpu.MemorySpace.HBM


def call(kernel, outs, args, scratch, flops, hbm_args=(), hbm_outs=()):
    def specs(count, in_hbm):
        return [pl.BlockSpec(memory_space=HBM if k in in_hbm else VMEM) for k in range(count)]

    args = [pltpu.with_memory_space_constraint(v, HBM) if k in hbm_args else v for k, v in enumerate(args)]
    return pl.pallas_call(
        kernel,
        out_shape=[(HBM if k in hbm_outs else jax.ShapeDtypeStruct)(s, d) for k, (s, d) in enumerate(outs)],
        in_specs=specs(len(args), hbm_args),
        out_specs=specs(len(outs), hbm_outs),
        scratch_shapes=scratch,
        cost_estimate=pl.CostEstimate(flops=flops, bytes_accessed=1 << 20, transcendentals=0),
        compiler_params=pltpu.CompilerParams(vmem_limit_bytes=VMEM_GRANT),
    )(*args)


def flat(groups):
    return [v for group in groups for v in group if v is not None]


def like(array):
    return pltpu.VMEM(array.shape, array.dtype)


def body(fields, trace_old, face_load, face_diag, fine_flag, coeff, volume_op, lift_op, schur_op):
    _, F, EX, EY, EZ = trace_old.shape
    geo = Geometry(F, EX, EY, EZ)
    M, dofs, N = geo.M, fields.shape[0], 6 * F
    devices = 1
    for a in AXES:
        devices *= lax.axis_size(a)
    n = counts()
    trace = trace_old.reshape(3 * F * M, EZ)
    load = face_load.reshape(3 * F * M, EZ)
    diag_in = face_diag.reshape(3 * M, EZ)
    fine = fine_flag.reshape(M, EZ)
    scale = coeff.reshape(M, EZ)
    nodal = fields.reshape(dofs * M, EZ)
    slab = [(EY, F, EZ), (EX, F, EZ)]
    slab_sent = [(EY * F, EZ), (EX * F, EZ)]
    slab_wide = [(EY * F + 8, EZ), (EX * F + 8, EZ)]
    full, pack, line = (3, M, F, EZ), (3, F, EZ), (8, EZ)
    halo_outs = [(s, f32) for s in slab]
    flops = 2 * 3 * N * N * M * EZ
    dma = pltpu.SemaphoreType.DMA

    def halves(blocks):
        return [pltpu.VMEM((N, blocks * EZ), bf16)] * 2

    def send_outs(shapes):
        return [(s, f32) for s, k in zip(shapes, n) for _ in range(k)]

    def grouped(values):
        values = list(values)
        return [[values.pop(0) for _ in range(k)] for k in n[:2]]

    held, sx, sy = call(functools.partial(kernel_slabs, geo), [(trace.shape, f32)] + [(s, f32) for s in slab_sent], [trace], [dma((1,))],
                        1 << 20, hbm_args=(0,))
    old = exchange(AXES[:2], [[sx, sx], [sy, sy]])
    own, diag, weight, schur, columns = call(
        functools.partial(kernel_prepare, geo),
        [(full, f32), ((3 * M, EZ), f32), ((M, EZ), f32), ((2 * N, N), bf16), ((3 * F + 8, EZ), f32)],
        [held, load, diag_in, fine, scale, schur_op], [like(load), like(fine), like(scale), like(schur_op), dma((5,))],
        flops, hbm_args=(1, 2, 3, 4, 5))
    base, lift = call(
        functools.partial(kernel_volume, geo), [((M, dofs, EZ), f32), (lift_op.shape, bf16)], [nodal, fine, volume_op, lift_op.T],
        [pltpu.VMEM((dofs * M, EZ), f32), like(nodal), like(fine), like(volume_op), like(lift_op.T), dma((4,))],
        2 * dofs * dofs * M * EZ, hbm_args=(0, 1, 2, 3))
    wide = call(functools.partial(kernel_pack, geo, n), [((4 * F + 8, EZ), f32)], [columns] + flat(old), [], 1 << 20)[0]
    got = exchange(AXES[2:], [[wide, wide]])
    out = call(functools.partial(kernel_start, geo, n),
               halo_outs + [(pack, f32), (line, f32), (full, f32), (pack, f32)] + send_outs(slab_wide),
               [held, own, weight, schur, base] + flat(old) + flat(got), halves(M + 1), flops)
    trace_pack, lines, partial, partial_pack, sent = out[2], out[3], out[4], out[5], grouped(out[6:])
    halo_old = [*out[:2], trace_pack]
    got = exchange(AXES[:2], sent)
    out = call(functools.partial(kernel_middle, geo, n),
               [(full, f32), ((F, EZ), f32)] + halo_outs + [(full, f32), ((F, EZ), f32)] + send_outs(slab_sent) + [((2, 8, EZ), f32)],
               [partial, partial_pack, diag, weight, schur, lines] + flat(sent) + flat(got), halves(M + 1), flops)
    r, r_z, partial, image_z, sent, dots = out[0], out[1], out[4], out[5], grouped(out[6:-1]), out[-1]
    halo_r = [*out[2:4], r_z]
    got = exchange(AXES[:2], sent)
    out = call(functools.partial(kernel_last, geo, n), [(full, f32)] + halo_outs + [((devices, EZ), f32)],
               [partial, image_z, diag, weight, schur, dots, r, *halo_r] + flat(sent) + flat(got), halves(M), flops)
    q, halo_q, message = out[0], [*out[1:3], image_z], out[3]
    message = lax.all_to_all(message, AXES, 0, 0, tiled=True)
    fields_new, trace_new = call(
        functools.partial(kernel_finish, geo), [((dofs * M, EZ), bf16), ((3 * F * M, EZ), f32)],
        [message, trace, base, fine, lift, r, q, *halo_old, *halo_r, *halo_q],
        [pltpu.VMEM((N, M * EZ), bf16), pltpu.VMEM((dofs * M, EZ), f32), like(nodal), like(trace), dma((PARTS + 1,))],
        2 * dofs * N * M * EZ, hbm_outs=(0, 1))
    return fields_new.reshape(fields.shape), trace_new.reshape(trace_old.shape)


def solution(mesh):
    placed = (
        P(None, *AXES), P(None, None, *AXES), P(None, None, *AXES), P(None, *AXES), P(*AXES), P(*AXES), P(), P(), P(),
    )
    return jax.shard_map(body, mesh=mesh, in_specs=placed, out_specs=(P(None, *AXES), P(None, None, *AXES)), check_vma=False)
```

```python
import functools

import jax
import jax.numpy as jnp
from jax import lax
from jax.experimental import pallas as pl
from jax.experimental.pallas import tpu as pltpu
from jax.sharding import PartitionSpec as P

AXES = ("gx", "gy", "gz")
TIME_STEP = 0.25
SHIFT_LIMIT = 1e4
PARTS = 4
STRIDE = 8
VMEM_GRANT = 12 * 1024 * 1024
f32, bf16 = jnp.float32, jnp.bfloat16


def pairs(axis, odd):
    size = lax.axis_size(axis)
    route = []
    for i in range(odd, size - 1, 2):
        route += [(i, i + 1), (i + 1, i)]
    return route


def exchange(axes, sends):
    return [[lax.ppermute(v, axis, pairs(axis, odd)) for odd, v in enumerate(s) if pairs(axis, odd)] for axis, s in zip(axes, sends)]


def counts():
    return [sum(bool(pairs(axis, odd)) for odd in (0, 1)) for axis in AXES]


def lane_iota(shape):
    return lax.broadcasted_iota(jnp.int32, shape, len(shape) - 1)


def moved(value, source, target):
    width = value.shape[-1]
    shift = (target - source) % width
    return pltpu.roll(value, shift, value.ndim - 1) if shift else value


def place():
    index = [lax.axis_index(a) for a in AXES]
    parity = [lax.rem(i, 2) for i in index]
    below_top = [(i < lax.axis_size(a) - 1).astype(f32) for i, a in zip(index, AXES)]
    return parity, below_top


def split(value):
    high = value.astype(bf16)
    return high, (value - high.astype(f32)).astype(bf16)


class Geometry:
    def __init__(self, F, EX, EY, EZ):
        self.F, self.EX, self.EY, self.EZ = F, EX, EY, EZ
        self.M = EX * EY


def at_rows(geo, s, m):
    return slice(s * geo.F, (s + 1) * geo.F), slice(m * geo.EZ, (m + 1) * geo.EZ)


def lanes_of(geo):
    lane = lane_iota((geo.F, geo.EZ))
    return lane, lane % STRIDE, lane // (STRIDE * geo.EY), (lane // STRIDE) % geo.EY


def part_of(geo, k, count):
    return slice(k * geo.F, k * geo.F + (geo.F if k < count else 8))


def fold(geo, a, value):
    lane = lane_iota((8, geo.EZ))
    unit = geo.EY * STRIDE if a == 0 else STRIDE
    slot = lane // unit if a == 0 else (lane % (geo.EY * STRIDE)) // unit
    out = jnp.zeros((8, geo.EZ), f32)
    for q in range(geo.F // 8):
        out = jnp.where(slot == q, moved(value[8 * q:8 * q + 8], 0, q * unit), out)
    return out


def unfold(geo, a, value):
    unit = geo.EY * STRIDE if a == 0 else STRIDE
    return jnp.concatenate([moved(value, q * unit, 0) for q in range(geo.F // 8)], 0)


def z_above(geo, z_own, z_pack, m):
    lane = lane_iota((geo.F, geo.EZ))
    return jnp.where(lane == geo.EZ - 1, moved(z_pack, m * STRIDE + 2, geo.EZ - 1), moved(z_own, 1, 0))


def gather_and_apply(geo, own, halo, schur, ghi, glo, wide=None):
    F, EX, EY, EZ, M = geo.F, geo.EX, geo.EY, geo.EZ, geo.M
    hx, hy, hz = halo

    def put(m, blocks):
        for s, block in enumerate(blocks):
            high, low = split(block)
            ghi[at_rows(geo, s, m)] = high
            glo[at_rows(geo, s, m)] = low

    bottom = jnp.zeros((F, EZ), f32)
    lane, column, at_i, at_j = lanes_of(geo)
    for m in range(M):
        i, j = divmod(m, EY)
        z_own = own(2, m)
        put(m, [
            own(0, m), own(0, m + EY) if i + 1 < EX else hx(j),
            own(1, m), own(1, m + 1) if j + 1 < EY else hy(i),
            z_own, z_above(geo, z_own, hz, m),
        ])
        if wide:
            bottom = jnp.where(lane == m * STRIDE + 1, moved(z_own, 0, m * STRIDE + 1), bottom)
    if wide:
        x, y, hx_pack, hy_pack = wide
        put(M, [
            x, jnp.where(at_i == EX - 1, moved(hx_pack, 0, (EX - 1) * EY * STRIDE), moved(x, EY * STRIDE, 0)),
            y, jnp.where(at_j == EY - 1, moved(hy_pack, 0, (EY - 1) * STRIDE), moved(y, STRIDE, 0)),
            hz, jnp.where(column == 1, bottom, moved(hz, 1, 0)),
        ])
    n = 6 * F
    both = jnp.dot(schur[...], ghi[...], preferred_element_type=f32)
    return both[:n] + (both[n:] + jnp.dot(schur[:n], glo[...], preferred_element_type=f32))


def spread(geo, y, weight, own_term, sign, out, sends, parity, weight_pack, own_pack, pack_out):
    F, EX, EY, EZ, M = geo.F, geo.EX, geo.EY, geo.EZ, geo.M
    lane, column, at_i, at_j = lanes_of(geo)
    wrow = [weight[m:m + 1] * sign for m in range(M)] + [weight_pack * sign]

    def block(s, m):
        return y[at_rows(geo, s, m)] * wrow[m]

    low = {}
    below = block(5, M)
    top = jnp.zeros((F, EZ), f32)
    for m in range(M):
        i, j = divmod(m, EY)
        vx = own_term(0, m) + block(0, m)
        if i > 0:
            vx = vx + block(1, m - EY)
        else:
            low[0, j] = vx
        out[0, m] = vx
        vy = own_term(1, m) + block(2, m)
        if j > 0:
            vy = vy + block(3, m - 1)
        else:
            low[1, i] = vy
        out[1, m] = vy
        up = block(5, m)
        out[2, m] = own_term(2, m) + block(4, m) + jnp.where(lane == 0, moved(below, m * STRIDE + 1, 0), moved(up, 0, 1))
        top = jnp.where(lane == m * STRIDE + 2, moved(up, EZ - 1, m * STRIDE + 2), top)
    shared = [
        [(low[0, j], block(1, (EX - 1) * EY + j)) for j in range(EY)],
        [(low[1, i], block(3, i * EY + EY - 1)) for i in range(EX)],
    ]
    pack_out[2][...] = own_pack(2) + block(4, M) + jnp.where(column == 2, top, moved(below, 0, 1))
    if 0 in pack_out:
        up = block(1, M)
        v = own_pack(0) + block(0, M)
        pack_out[0][...] = v + jnp.where(at_i > 0, moved(up, 0, EY * STRIDE), 0.0)
        shared[0].append((fold(geo, 0, v), fold(geo, 0, moved(up, (EX - 1) * EY * STRIDE, 0))))
        up = block(3, M)
        v = own_pack(1) + block(2, M)
        pack_out[1][...] = v + jnp.where(at_j > 0, moved(up, 0, STRIDE), 0.0)
        shared[1].append((fold(geo, 1, v), fold(geo, 1, moved(up, (EY - 1) * STRIDE, 0))))
    for a in (0, 1):
        for odd, ref in enumerate(sends[a]):
            for k, (bottom, high) in enumerate(shared[a]):
                ref[part_of(geo, k, (EY, EX)[a])] = jnp.where(parity[a] == odd, high, bottom)


def chosen(refs, parity, read, flip=False):
    values = [read(r) for r in refs]
    if not values:
        return None
    if len(values) == 1:
        values.append(jnp.zeros_like(values[0]))
    first, second = (values[1], values[0]) if flip else values
    return jnp.where(parity == 0, first, second)


def completed(geo, partial, sent, got, parity, below_top, full, halos):
    F, EX, EY, EZ, M = geo.F, geo.EX, geo.EY, geo.EZ, geo.M
    for f in range(3):
        for m in range(M):
            i, j = divmod(m, EY)
            v = partial[f, m]
            if f == 0 and i == 0 and got[0]:
                v = v + chosen(got[0], parity[0], lambda r: r[part_of(geo, j, EY)], True)
            if f == 1 and j == 0 and got[1]:
                v = v + chosen(got[1], parity[1], lambda r: r[part_of(geo, i, EX)], True)
            full[f, m] = v
    for a, n in ((0, EY), (1, EX)):
        for k in range(n):
            halos[a][k] = both_sides(geo, sent[a], got[a], parity[a], below_top[a], part_of(geo, k, n))


def both_sides(geo, sent, got, parity, below_top, k):
    if not got:
        return jnp.zeros((k.stop - k.start, geo.EZ), f32)
    return (chosen(sent, parity, lambda r: r[k]) + chosen(got, parity, lambda r: r[k])) * below_top


def folded(total, value):
    v = value.reshape(value.shape[0] // 8, 8, value.shape[1]).sum(0)
    return v if total is None else total + v


def rows(ref, geo, f, m):
    return ref[pl.ds(f * geo.F * geo.M + m, geo.F, stride=geo.M), :]


def kernel_slabs(geo, trace, held, sx, sy, sems):
    for c in fetch([(trace, held)], sems):
        c.wait()
    for f, (ref, count, step) in enumerate(((sx, geo.EY, 1), (sy, geo.EX, geo.EY))):
        for k in range(count):
            ref[part_of(geo, k, count)] = rows(held, geo, f, k * step)


def packed(geo, parts, start=0, out=None, spread=1):
    slot = lane_iota(parts[0].shape) // STRIDE
    out = jnp.zeros(parts[0].shape, f32) if out is None else out
    for k, part in enumerate(parts):
        at = start + k * spread * STRIDE
        out = jnp.where(slot == at // STRIDE, moved(part, 0, at + 2), out)
    return out


def kernel_pack(geo, n, columns, *refs):
    got, (out,) = take(refs, n[:2], 1)
    parity, _ = place()
    rows_in = columns.shape[0]
    out[:rows_in] = columns[...]
    for a, count, spread in ((0, geo.EY, 1), (1, geo.EX, geo.EY)):
        block = jnp.zeros((geo.F, geo.EZ), f32)
        if got[a]:
            parts = [chosen(got[a], parity[a], lambda r: r[part_of(geo, k, count)]) for k in range(count)]
            block = packed(geo, parts, 0, block, spread)
        out[rows_in + 8 * a:rows_in + 8 * a + 8] = fold(geo, a, block)


def take(refs, *sizes):
    refs = list(refs)
    out = []
    for s in sizes:
        if isinstance(s, (list, tuple)):
            group = []
            for n in s:
                group.append([refs.pop(0) for _ in range(n)])
            out.append(group)
        else:
            out.append([refs.pop(0) for _ in range(s)])
    assert not refs
    return out


def fetch(pairs, sems):
    copies = [pltpu.make_async_copy(src, dst, sems.at[k]) for k, (src, dst) in enumerate(pairs)]
    for c in copies:
        c.start()
    return copies


def kernel_prepare(geo, trace, load, diag_in, fine, coeff, schur, own, diag, weight, matrix, columns, vload, vfine, vcoeff, vschur, sems):
    F, M = geo.F, geo.M
    copies = fetch([(load, vload), (diag_in, diag), (fine, vfine), (coeff, vcoeff), (schur, vschur)], sems)
    for c in copies:
        c.wait()
    scale = vfine[...].astype(f32) * vcoeff[...]
    weight[...] = scale
    n = 6 * F
    matrix[:n], matrix[n:] = split(vschur[...])
    for f in range(3):
        for m in range(M):
            own[f, m] = rows(vload, geo, f, m) - diag[f * M + m:f * M + m + 1] * rows(trace, geo, f, m)
        old = packed(geo, [rows(trace, geo, f, m) for m in range(M)])
        columns[f * F:(f + 1) * F] = packed(geo, [own[f, m] for m in range(M)], geo.EZ // 2, old)
    lines = [packed(geo, [diag[f * M + m:f * M + m + 1] for m in range(M)]) for f in range(3)]
    lines.append(packed(geo, [scale[m:m + 1] for m in range(M)]))
    for k in range(8):
        columns[3 * F + k:3 * F + k + 1] = lines[min(k, 3)]


def kernel_start(geo, n, trace, own, weight, schur, _, *refs):
    got, halos, (trace_pack, lines, partial, partial_pack), sends, (ghi, glo) = take(refs, n, 2, 4, n[:2], 2)
    F, EX, EY, EZ = geo.F, geo.EX, geo.EY, geo.EZ
    parity, _ = place()
    lane = lane_iota((F, EZ))

    def mixed(rows_at):
        if not got[2]:
            return jnp.zeros((rows_at.stop - rows_at.start, EZ), f32)
        below = chosen(got[2], parity[2], lambda r: r[rows_at], True)
        above = chosen(got[2], parity[2], lambda r: r[rows_at])
        return jnp.where(lane[:below.shape[0]] % STRIDE < 2, below, above)

    lines[...] = mixed(slice(3 * F, 3 * F + 8))
    own_pack = []
    for f in range(3):
        v = mixed(slice(f * F, (f + 1) * F))
        trace_pack[f] = jnp.where(lane < EZ // 2, v, 0.0)
        own_pack.append(jnp.where(lane < EZ // 2, moved(v, EZ // 2, 0), 0.0))
    beside = [unfold(geo, a, mixed(slice(3 * F + 8 + 8 * a, 3 * F + 16 + 8 * a))) for a in (0, 1)]
    for a, count in ((0, EY), (1, EX)):
        for k in range(count):
            halos[a][k] = chosen(got[a], parity[a], lambda r: r[part_of(geo, k, count)]) if got[a] else jnp.zeros((F, EZ), f32)
    halo = (lambda j: halos[0][j], lambda i: halos[1][i], trace_pack[2])
    wide = (trace_pack[0], trace_pack[1], *beside)
    y = gather_and_apply(geo, lambda f, m: rows(trace, geo, f, m), halo, schur, ghi, glo, wide)
    spread(geo, y, weight[...], lambda f, m: own[f, m], -1.0, partial, sends, parity,
           lines[3:4], lambda f: own_pack[f], {f: partial_pack.at[f] for f in range(3)})


def accumulate(total, value):
    return value if total is None else total + value


def kernel_middle(geo, n, partial, partial_pack, diag, weight, schur, lines, *refs):
    sent, got, (full, full_z), halos, (image, image_z), sends, (dots,), (ghi, glo) = take(refs, n[:2], n[:2], 2, 2, 2, n[:2], 1, 2)
    F, EX, EY, EZ, M = geo.F, geo.EX, geo.EY, geo.EZ, geo.M
    parity, below_top = place()
    completed(geo, partial, sent, got, parity, below_top, full, halos)
    lane, column, at_i, at_j = lanes_of(geo)
    packs = []
    for a, edge, count in ((0, at_i == 0, EY), (1, at_j == 0, EX)):
        v = partial_pack[a]
        if got[a]:
            v = v + jnp.where(edge, unfold(geo, a, chosen(got[a], parity[a], lambda r: r[part_of(geo, count, count)], True)), 0.0)
        packs.append(v)
    beside = [unfold(geo, a, both_sides(geo, sent[a], got[a], parity[a], below_top[a], part_of(geo, k, k))) for a, k in ((0, EY), (1, EX))]
    wide = (*packs, *beside)
    full_z[...] = jnp.where(column < 2, partial_pack[2], partial_pack[2] * below_top[2])
    halo = (lambda j: halos[0][j], lambda i: halos[1][i], full_z[...])
    y = gather_and_apply(geo, lambda f, m: full[f, m], halo, schur, ghi, glo, wide)
    squares = energy = None
    for f in range(3):
        for m in range(M):
            vv = folded(None, full[f, m] * full[f, m])
            squares = accumulate(squares, vv)
            energy = accumulate(energy, vv * diag[f * M + m:f * M + m + 1])
    for m in range(M):
        part = None
        for s in range(6):
            at = at_rows(geo, s, m)
            part = folded(part, (ghi[at].astype(f32) + glo[at].astype(f32)) * y[at])
        energy = energy + part * weight[m:m + 1]
    dots[0], dots[1] = squares, energy
    spread(geo, y, weight[...], lambda f, m: diag[f * M + m:f * M + m + 1] * full[f, m], 1.0, image, sends, parity,
           lines[3:4], lambda f: lines[f:f + 1] * full_z[...], {2: image_z})
    image_z[...] = image_z[...] * below_top[2]


def kernel_last(geo, n, partial, image_z, diag, weight, schur, dots, r, hxr, hyr, hzr, *refs):
    sent, got, (full,), halos, (message,), (ghi, glo) = take(refs, n[:2], n[:2], 1, 2, 1, 2)
    F, EX, EY, EZ, M = geo.F, geo.EX, geo.EY, geo.EZ, geo.M
    parity, below_top = place()
    completed(geo, partial, sent, got, parity, below_top, full, halos)
    along = None
    for f in range(3):
        for m in range(M):
            along = folded(along, r[f, m] * full[f, m])
    squares = jnp.sum(dots[0], keepdims=True)
    along = jnp.sum(along, keepdims=True)
    shift = jnp.where(squares > 0, jnp.clip(along / squares, -SHIFT_LIMIT, SHIFT_LIMIT), 0.0)
    halo = (lambda j: halos[0][j] - shift * hxr[j], lambda i: halos[1][i] - shift * hyr[i], image_z[...] - shift * hzr[...])
    y = gather_and_apply(geo, lambda f, m: full[f, m] - shift * r[f, m], halo, schur, ghi, glo)
    rp = pp = erp = epp = None
    for f in range(3):
        for m in range(M):
            v = r[f, m]
            p = full[f, m] - shift * v
            d = diag[f * M + m:f * M + m + 1]
            a, b = folded(None, v * p), folded(None, p * p)
            rp, pp = accumulate(rp, a), accumulate(pp, b)
            erp, epp = accumulate(erp, a * d), accumulate(epp, b * d)
    for m in range(M):
        i, j = divmod(m, EY)
        blocks = [
            r[0, m], r[0, m + EY] if i + 1 < EX else hxr[j],
            r[1, m], r[1, m + 1] if j + 1 < EY else hyr[i],
            r[2, m], z_above(geo, r[2, m], hzr[...], m),
        ]
        one = two = None
        for s, block in enumerate(blocks):
            at = at_rows(geo, s, m)
            one = folded(one, block * y[at])
            two = folded(two, (ghi[at].astype(f32) + glo[at].astype(f32)) * y[at])
        erp = erp + one * weight[m:m + 1]
        epp = epp + two * weight[m:m + 1]
    lane = lane_iota((1, EZ))
    line = jnp.where(lane == 0, shift, jnp.where(lane == 1, squares, 0.0))
    for k, v in enumerate((rp, pp, dots[1], erp, epp)):
        line = jnp.where(lane == k + 2, jnp.sum(v, keepdims=True), line)
    message[...] = jnp.broadcast_to(line, message.shape)


def step_sizes(rows_of_devices):
    lanes = lane_iota(rows_of_devices.shape)
    theta, rr, rp, pp, err, erp, epp = [jnp.sum(jnp.where(lanes == k, rows_of_devices, 0.0), 1, keepdims=True) for k in range(7)]

    def total(v):
        return jnp.sum(v, 0, keepdims=True)

    old = total(rr)
    alpha = old / total(err)
    u = 1.0 - alpha * theta
    new = total(u * u * rr - 2.0 * u * alpha * rp + alpha * alpha * pp)
    beta = new / old
    c = u + beta
    energy = total(c * c * err - 2.0 * c * alpha * erp + alpha * alpha * epp)
    second = jnp.where(energy > 0, new / energy, 0.0)
    return alpha + second * (1.0 + beta), -alpha * second


def kernel_volume(geo, fields, fine, operator, lift_in, base, lift, plain, vfields, vfine, voperator, vlift, sems):
    M, EZ = geo.M, geo.EZ
    dofs = operator.shape[0]
    for c in fetch([(fields, vfields), (fine, vfine), (operator, voperator), (lift_in, vlift)], sems):
        c.wait()
    plain[...] = vfields[...].astype(f32)
    lift[...] = vlift[...].T
    nodal = [plain[pl.ds(m, dofs, stride=M), :] for m in range(M)]
    volume = jnp.dot(voperator[...], jnp.concatenate([v.astype(bf16) for v in nodal], 1), preferred_element_type=f32)
    coarse = 1.0 - vfine[...].astype(f32)
    for m in range(M):
        base[m] = nodal[m] + (TIME_STEP * coarse[m:m + 1]) * volume[:, m * EZ:(m + 1) * EZ]


def kernel_finish(geo, message, trace, base, fine, lift, r, q, *refs):
    (hx, hy, hz), (hxr, hyr, hzr), (hxq, hyq, hzq), (fields_out, trace_out), (g, plain, fields_new, trace_new, sems) = take(refs, 3, 3, 3, 2, 5)
    F, EX, EY, EZ, M = geo.F, geo.EX, geo.EY, geo.EZ, geo.M
    cr, cq = step_sizes(message[...])
    flag = fine[...].astype(f32)
    z_step = cr * hzr[...] + cq * hzq[...]
    for m in range(M):
        i, j = divmod(m, EY)
        mark = flag[m:m + 1]

        def old_step(f, k):
            return rows(trace, geo, f, k), cr * r[f, k] + cq * q[f, k]

        ox, sx = old_step(0, m)
        oy, sy = old_step(1, m)
        oz, sz = old_step(2, m)
        for f, (o, s) in enumerate(((ox, sx), (oy, sy), (oz, sz))):
            trace_new[pl.ds(f * F * M + m, F, stride=M), :] = o + s
        up_x = old_step(0, m + EY) if i + 1 < EX else (hx[j], cr * hxr[j] + cq * hxq[j])
        up_y = old_step(1, m + 1) if j + 1 < EY else (hy[i], cr * hyr[i] + cq * hyq[i])
        up_z = (z_above(geo, oz, hz[2], m), z_above(geo, sz, z_step, m))
        for s, (o, step) in enumerate(((ox, sx), up_x, (oy, sy), up_y, (oz, sz), up_z)):
            g[s * F:(s + 1) * F, m * EZ:(m + 1) * EZ] = (o + mark * step).astype(bf16)
    copies = [pltpu.make_async_copy(trace_new, trace_out, sems.at[0])]
    copies[0].start()
    dofs = lift.shape[0]
    part = dofs // PARTS
    for k in range(PARTS):
        lifted = jnp.dot(lift[k * part:(k + 1) * part], g[...], preferred_element_type=f32)
        for m in range(M):
            plain[pl.ds(k * part * M + m, part, stride=M), :] = base[m, k * part:(k + 1) * part] + TIME_STEP * lifted[:, m * EZ:(m + 1) * EZ]
        some = pl.ds(k * part * M, part * M)
        fields_new[some] = plain[some].astype(bf16)
        copies.append(pltpu.make_async_copy(fields_new.at[some], fields_out.at[some], sems.at[k + 1]))
        copies[-1].start()
    for c in copies:
        c.wait()


VMEM, HBM = pltpu.MemorySpace.VMEM, pltpu.MemorySpace.HBM


def call(kernel, outs, args, scratch, flops, hbm_args=(), hbm_outs=()):
    def specs(count, in_hbm):
        return [pl.BlockSpec(memory_space=HBM if k in in_hbm else VMEM) for k in range(count)]

    args = [pltpu.with_memory_space_constraint(v, HBM) if k in hbm_args else v for k, v in enumerate(args)]
    return pl.pallas_call(
        kernel,
        out_shape=[(HBM if k in hbm_outs else jax.ShapeDtypeStruct)(s, d) for k, (s, d) in enumerate(outs)],
        in_specs=specs(len(args), hbm_args),
        out_specs=specs(len(outs), hbm_outs),
        scratch_shapes=scratch,
        cost_estimate=pl.CostEstimate(flops=flops, bytes_accessed=1 << 20, transcendentals=0),
        compiler_params=pltpu.CompilerParams(vmem_limit_bytes=VMEM_GRANT),
    )(*args)


def flat(groups):
    return [v for group in groups for v in group if v is not None]


def like(array):
    return pltpu.VMEM(array.shape, array.dtype)


def body(fields, trace_old, face_load, face_diag, fine_flag, coeff, volume_op, lift_op, schur_op):
    _, F, EX, EY, EZ = trace_old.shape
    geo = Geometry(F, EX, EY, EZ)
    M, dofs, N = geo.M, fields.shape[0], 6 * F
    devices = 1
    for a in AXES:
        devices *= lax.axis_size(a)
    n = counts()
    trace = trace_old.reshape(3 * F * M, EZ)
    load = face_load.reshape(3 * F * M, EZ)
    diag_in = face_diag.reshape(3 * M, EZ)
    fine = fine_flag.reshape(M, EZ)
    scale = coeff.reshape(M, EZ)
    nodal = fields.reshape(dofs * M, EZ)
    slab = [(EY, F, EZ), (EX, F, EZ)]
    slab_sent = [(EY * F, EZ), (EX * F, EZ)]
    slab_wide = [(EY * F + 8, EZ), (EX * F + 8, EZ)]
    full, pack, line = (3, M, F, EZ), (3, F, EZ), (8, EZ)
    halo_outs = [(s, f32) for s in slab]
    flops = 2 * 3 * N * N * M * EZ
    dma = pltpu.SemaphoreType.DMA

    def halves(blocks):
        return [pltpu.VMEM((N, blocks * EZ), bf16)] * 2

    def send_outs(shapes):
        return [(s, f32) for s, k in zip(shapes, n) for _ in range(k)]

    def grouped(values):
        values = list(values)
        return [[values.pop(0) for _ in range(k)] for k in n[:2]]

    held, sx, sy = call(functools.partial(kernel_slabs, geo), [(trace.shape, f32)] + [(s, f32) for s in slab_sent], [trace], [dma((1,))],
                        1 << 20, hbm_args=(0,))
    old = exchange(AXES[:2], [[sx, sx], [sy, sy]])
    own, diag, weight, schur, columns = call(
        functools.partial(kernel_prepare, geo),
        [(full, f32), ((3 * M, EZ), f32), ((M, EZ), f32), ((2 * N, N), bf16), ((3 * F + 8, EZ), f32)],
        [held, load, diag_in, fine, scale, schur_op], [like(load), like(fine), like(scale), like(schur_op), dma((5,))],
        flops, hbm_args=(1, 2, 3, 4, 5))
    base, lift = call(
        functools.partial(kernel_volume, geo), [((M, dofs, EZ), f32), (lift_op.shape, bf16)], [nodal, fine, volume_op, lift_op.T],
        [pltpu.VMEM((dofs * M, EZ), f32), like(nodal), like(fine), like(volume_op), like(lift_op.T), dma((4,))],
        2 * dofs * dofs * M * EZ, hbm_args=(0, 1, 2, 3))
    wide = call(functools.partial(kernel_pack, geo, n), [((3 * F + 24, EZ), f32)], [columns] + flat(old), [], 1 << 20)[0]
    got = exchange(AXES[2:], [[wide, wide]])
    out = call(functools.partial(kernel_start, geo, n),
               halo_outs + [(pack, f32), (line, f32), (full, f32), (pack, f32)] + send_outs(slab_wide),
               [held, own, weight, schur, base] + flat(old) + flat(got), halves(M + 1), flops)
    trace_pack, lines, partial, partial_pack, sent = out[2], out[3], out[4], out[5], grouped(out[6:])
    halo_old = [*out[:2], trace_pack]
    got = exchange(AXES[:2], sent)
    out = call(functools.partial(kernel_middle, geo, n),
               [(full, f32), ((F, EZ), f32)] + halo_outs + [(full, f32), ((F, EZ), f32)] + send_outs(slab_sent) + [((2, 8, EZ), f32)],
               [partial, partial_pack, diag, weight, schur, lines] + flat(sent) + flat(got), halves(M + 1), flops)
    r, r_z, partial, image_z, sent, dots = out[0], out[1], out[4], out[5], grouped(out[6:-1]), out[-1]
    halo_r = [*out[2:4], r_z]
    got = exchange(AXES[:2], sent)
    out = call(functools.partial(kernel_last, geo, n), [(full, f32)] + halo_outs + [((devices, EZ), f32)],
               [partial, image_z, diag, weight, schur, dots, r, *halo_r] + flat(sent) + flat(got), halves(M), flops)
    q, halo_q, message = out[0], [*out[1:3], image_z], out[3]
    message = lax.all_to_all(message, AXES, 0, 0, tiled=True)
    fields_new, trace_new = call(
        functools.partial(kernel_finish, geo), [((dofs * M, EZ), bf16), ((3 * F * M, EZ), f32)],
        [message, trace, base, fine, lift, r, q, *halo_old, *halo_r, *halo_q],
        [pltpu.VMEM((N, M * EZ), bf16), pltpu.VMEM((dofs * M, EZ), f32), like(nodal), like(trace), dma((PARTS + 1,))],
        2 * dofs * N * M * EZ, hbm_outs=(0, 1))
    return fields_new.reshape(fields.shape), trace_new.reshape(trace_old.shape)


def solution(mesh):
    placed = (
        P(None, *AXES), P(None, None, *AXES), P(None, None, *AXES), P(None, *AXES), P(*AXES), P(*AXES), P(), P(), P(),
    )
    return jax.shard_map(body, mesh=mesh, in_specs=placed, out_specs=(P(None, *AXES), P(None, None, *AXES)), check_vma=False)
```
